32 devices in a mesh: ctx: 8 (over y, x, core), tp: 4 (over z).
Axes of the slice: x: 2, y: 2, z: 4, core: 2. Of those that a mesh axis runs over, the one named last changes fastest.
Arguments:
- queries: bfloat16 [2048, 8192], P('ctx', 'tp'), may hold values from -8 to 8
- keys: bfloat16 [2048, 1024], P('ctx'), may hold values from -6 to 6
- values: bfloat16 [2048, 1024], P('ctx'), may hold values from -6 to 6
Outputs:
- attended: bfloat16 [2048, 8192], P('ctx', 'tp')
The draws below stay inside these ranges and needn't reach their ends.
All inputs are finite; a program needn't handle non-finite values.
Results may differ from the reference program's by a relative error of at most 0.0032.
Values may be sent and summed in bfloat16 or wider, within the bound.
A program may use at most 64 MiB of HBM per device.

```python
import jax
import jax.numpy as jnp
from jax import lax

HEADS = 64
KV_HEADS = 8
HEAD_DIM = 128
TOKENS = 2048


def draw_keys(key, part):
    drawn = jnp.clip(jax.random.normal(jax.random.fold_in(key, 11), (TOKENS, KV_HEADS * HEAD_DIM), jnp.float32), -6.0, 6.0)
    return drawn.astype(jnp.bfloat16)


def draw_queries(key, part):
    drawn = jnp.clip(2.5 * jax.random.normal(jax.random.fold_in(key, 13), (TOKENS, HEADS * HEAD_DIM), jnp.float32), -8.0, 8.0)
    return drawn.astype(jnp.bfloat16)


def block_levels(stream_key, dims, pieces, least, high):
    factor_of, own = 1.0, jax.random.fold_in(stream_key, 6)
    for dim, blocks in pieces:
        draws = jnp.exp(jax.random.uniform(jax.random.fold_in(own, dim), (blocks,), jnp.float32, least / len(pieces), high / len(pieces)))
        factor_of = factor_of * jnp.repeat(draws, dims[dim] // blocks).reshape([-1 if axis == dim else 1 for axis in range(len(dims))])
    return factor_of


def gaussian(rng, extent, width, most, pieces=(), held_as=jnp.bfloat16):
    entries = jax.random.normal(rng, extent, jnp.float32) * width
    if len(pieces) > 0:
        entries = block_levels(rng, extent, pieces, -0.22, 0.18) * entries
    return jnp.clip(entries, min=-most, max=most).astype(held_as)


def setup_inputs(seed: int = 0) -> dict:
    splits = jax.random.split(jax.random.key(seed), 4)
    return {
        "queries": draw_queries(jax.random.fold_in(splits[3], 71), 0),
        "keys": draw_keys(jax.random.fold_in(splits[3], 71), 0),
        "values": gaussian(splits[2], (TOKENS, KV_HEADS * HEAD_DIM), 1.0, 6.0, ((0, 8),)),
    }


def attention(queries, keys, values):
    group_size = HEADS // KV_HEADS
    score_scale = HEAD_DIM ** -0.5
    token_positions = jnp.arange(TOKENS, dtype=jnp.int32)
    allowed = token_positions[None, :] <= token_positions[:, None]

    def one_head(head_index):
        kv_index = head_index // group_size
        query_head = lax.dynamic_slice_in_dim(queries, head_index * HEAD_DIM, HEAD_DIM, 1)
        key_head = lax.dynamic_slice_in_dim(keys, kv_index * HEAD_DIM, HEAD_DIM, 1)
        value_head = lax.dynamic_slice_in_dim(values, kv_index * HEAD_DIM, HEAD_DIM, 1)
        scores = jnp.dot(query_head, key_head.T, preferred_element_type=jnp.float32) * score_scale
        scores = jnp.where(allowed, scores, -jnp.inf)
        row_peak = jnp.max(scores, axis=1, keepdims=True)
        raw_weights = jnp.where(allowed, jnp.exp(scores - row_peak), 0.0)
        row_total = jnp.sum(raw_weights, axis=1, keepdims=True)
        weights = raw_weights.astype(jnp.bfloat16)
        summed = jnp.dot(weights, value_head, preferred_element_type=jnp.float32)
        return (summed / row_total).astype(jnp.bfloat16)

    per_head = lax.map(one_head, jnp.arange(HEADS, dtype=jnp.int32))
    return jnp.transpose(per_head, (1, 0, 2)).reshape(TOKENS, HEADS * HEAD_DIM)


def reference(queries, keys, values):
    return attention(queries, keys, values)
```

```python
import functools
import math

import jax
import jax.numpy as jnp
from jax import lax
from jax.experimental import pallas as pl
from jax.experimental.pallas import tpu as pltpu
from jax.sharding import PartitionSpec as P

HEADS = 64
KV_HEADS = 8
HEAD_DIM = 128
LANES = 128
MASKED = -1e30
CHUNK = 8
DEPTH = 1
ROUTED = 1
EXP2_SCALE = HEAD_DIM ** -0.5 * math.log2(math.e)


def attend_heads(q_v, kv, acc, peak, heads, kv_head, blocks, masked, first):
    k = jnp.concatenate([kv[b, kv_head, 0] for b in blocks], 0)
    v = jnp.concatenate([kv[b, kv_head, 1] for b in blocks], 0)
    v = jnp.concatenate([v, jnp.ones((v.shape[0], LANES), v.dtype)], 1)
    rows, count = q_v.shape[0], k.shape[0]

    def score(h):
        q = q_v[:, pl.ds(pl.multiple_of(h * HEAD_DIM, HEAD_DIM), HEAD_DIM)]
        return lax.dot_general(q, k, (((1,), (1,)), ((), ())), preferred_element_type=jnp.float32)

    def fold(h, s):
        if masked:
            row = lax.broadcasted_iota(jnp.int32, s.shape, 0)
            col = lax.broadcasted_iota(jnp.int32, s.shape, 1)
            s = jnp.where(col <= row, s, MASKED)
        top = jnp.broadcast_to(jnp.max(s, axis=1, keepdims=True), (rows, LANES))
        if not first:
            before = peak[h]
            top = jnp.maximum(before, top)
        peak[h] = top
        wide = jnp.concatenate([top] * (count // LANES), 1)
        w = jnp.exp2((s - wide) * EXP2_SCALE).astype(jnp.bfloat16)
        new = jnp.dot(w, v, preferred_element_type=jnp.float32)
        if not first:
            shrink = jnp.exp2((before - top) * EXP2_SCALE)
            new = acc[h] * jnp.concatenate([shrink, shrink], 1) + new
        acc[h] = new

    ahead = [score(h) for h in heads[:DEPTH]]
    for i, h in enumerate(heads):
        if i + DEPTH < len(heads):
            ahead.append(score(heads[i + DEPTH]))
        fold(h, ahead.pop(0))


def kernel(nc, per_dev, group, kv_dev, q_hbm, k_hbm, v_hbm, o_ref,
           q_v, kv, acc, peak, loc_sem, send_sem, fwd_sem, far_sem, recv_sem):
    c = lax.axis_index("ctx")
    tp = lax.axis_index("tp")
    odd = lax.rem(c, 2)
    pair = c // 2
    partner = c + 1 - 2 * odd
    shared = per_dev // kv_dev
    chunk = min(CHUNK, shared)
    square = nc == 8 and kv_dev == 2
    base = tp * per_dev // group

    loads = []
    for g in range(kv_dev):
        cols = pl.ds(pl.multiple_of((base + g) * HEAD_DIM, HEAD_DIM), HEAD_DIM)
        loads.append([
            pltpu.make_async_copy(ref.at[:, cols], kv.at[c, g, i], loc_sem.at[2 * g + i])
            for i, ref in enumerate((k_hbm, v_hbm))])
        for load in loads[g]:
            load.start()
    load_q = pltpu.make_async_copy(q_hbm, q_v, loc_sem.at[2 * kv_dev])
    load_q.start()

    barrier = pltpu.get_barrier_semaphore()
    pl.semaphore_signal(barrier, inc=1, device_id={"ctx": partner})
    for i in range(1, nc // 2):
        pl.semaphore_signal(barrier, inc=1, device_id={"ctx": lax.rem(c + 2 * i, nc)})
    pl.semaphore_wait(barrier, nc // 2)

    def copy_to(b, g, target, sem):
        return pltpu.make_async_remote_copy(
            src_ref=kv.at[b, g], dst_ref=kv.at[b, g], send_sem=sem, recv_sem=recv_sem.at[b, g],
            device_id={"ctx": target})

    for load in sum(loads, []):
        load.wait()
    sends, late = [], []
    for g in range(kv_dev):
        sends.append((odd == 0, copy_to(c, g, partner, send_sem.at[0, g])))
        if square:
            beside = copy_to(c, g, lax.rem(c + 2, nc), send_sem.at[1, g])
            sends.append((lax.rem(pair, 2) == 0, beside))
            if g >= ROUTED:
                late.append(beside)
            first = kv_dev - 1 - g
            other = lax.select(pair == 0, first, g)
            sends.append((pair < 2, copy_to(c, other, lax.rem(c + 4, nc), send_sem.at[2, g])))
        else:
            for i in range(1, nc // 2):
                sends.append((c + 2 * i < nc, copy_to(c, g, lax.rem(c + 2 * i, nc), send_sem.at[i, g])))
    for wanted, copy in sends:
        pl.when(wanted)(copy.start)
    load_q.wait()

    def item(t):
        if not square:
            return pair - 1 - t // kv_dev, lax.rem(t, kv_dev)
        third = (lax.select(t < 4, 2 - lax.rem(t, 2), 0), lax.select(t < 4, t // 2, t - 4))
        second = (t // 2, lax.rem((t + 1) // 2 + 1, 2))
        return (lax.select(pair == 3, third[0], lax.select(pair == 2, second[0], 0)),
                lax.select(pair == 3, third[1], lax.select(pair == 2, second[1], t)))

    def onward(p, g):
        mine = 2 * p + odd
        up = ((pair == 1) & (g == 0)) | ((pair == 2) & (p == 0) & (g == 1))
        back = (pair == 3) & (p == 1) & (g < ROUTED)
        target = lax.select(pair == 3, 4 + odd, 6 + odd)
        return up | back, copy_to(mine, g, target, far_sem.at[p, g])

    def pull(t):
        p, g = item(t)
        copy = copy_to(2 * p + odd, g, partner, fwd_sem.at[p, g])
        copy.wait_recv()
        if square:
            wanted, far = onward(p, g)
            pl.when(wanted)(far.start)
        copy.start()

    def sweep(blocks, kv_head, masked, first):
        def body(n, carry):
            heads = [n * chunk + i for i in range(chunk)]
            g = n * chunk // shared if kv_head is None else kv_head
            attend_heads(q_v, kv, acc, peak, heads, g, blocks, masked, first)
            return carry
        return body

    def finish(g, carry):
        for i in range(shared):
            h = g * shared + i
            out = acc[h, :, :LANES] / acc[h, :, LANES:]
            o_ref[:, pl.ds(pl.multiple_of(h * HEAD_DIM, HEAD_DIM), HEAD_DIM)] = out.astype(o_ref.dtype)
        return carry

    chunks = per_dev // chunk
    steps = pair * kv_dev
    lax.fori_loop(0, chunks, sweep([c], None, True, True), 0)

    if square:
        for copy in late:
            pl.when(pair == 1)(copy.start)

    def first_pulls():
        pull(0)
        if square:
            pl.when(pair == 3)(functools.partial(pull, 1))

    @pl.when(odd == 1)
    def _():
        for g in range(kv_dev):
            copy_to(c - 1, g, partner, send_sem.at[0, g]).wait_recv()
        work = sweep([c - 1], None, False, False)

        def body(n, carry):
            pl.when((n == chunks // 2) & (pair > 0))(first_pulls)
            return work(n, carry)

        lax.fori_loop(0, chunks, body, 0)

    pl.when((odd == 0) & (pair > 0))(first_pulls)

    def step(t, carry):
        p, g = item(t)
        copy_to(2 * p + 1 - odd, g, partner, fwd_sem.at[p, g]).wait_recv()
        body = sweep([2 * p, 2 * p + 1], g, False, False)

        done = (pair == 3) & (t == 0) if square else False

        @pl.when((t + 1 < steps) & jnp.logical_not(done))
        def _():
            pull(t + 1)

        per_head = shared // chunk
        lax.fori_loop(g * per_head, (g + 1) * per_head, body, 0)

        @pl.when(t >= steps - kv_dev)
        def _():
            finish(g, 0)
        return carry

    lax.fori_loop(0, steps, step, 0)

    @pl.when(pair == 0)
    def _():
        lax.fori_loop(0, kv_dev, finish, 0)

    def drain(t, carry):
        p, g = item(t)
        copy_to(2 * p + odd, g, partner, fwd_sem.at[p, g]).wait_send()
        if square:
            wanted, far = onward(p, g)
            pl.when(wanted)(far.wait_send)
        return carry

    lax.fori_loop(0, steps, drain, 0)
    for wanted, copy in sends:
        pl.when(wanted)(copy.wait_send)
    for copy in late:
        pl.when(pair == 1)(copy.wait_send)


AHEAD = 4
LAG = 4
HOLD = 2
RING = 8
SUMS = 16


def paired_kernel(shared, q_hbm, k_hbm, v_hbm, o_ref, q_raw, q_t, kv, other, acc, peak, shrink,
                  ring, v_t, stage, load_sem, pair_sem, send_sem, relay_sem, recv_sem, out_sem):
    c = lax.axis_index("ctx")
    tp = lax.axis_index("tp")
    o = lax.rem(c, 2)
    chip = c // 2
    partner = c + 1 - 2 * o
    rows = q_raw.shape[1]
    half = rows // 2
    span = shared * HEAD_DIM
    tiles = 2 * shared
    f32, bf16 = jnp.float32, jnp.bfloat16

    def head_cols(g, width):
        return pl.ds(pl.multiple_of(g * width, width), width)

    loads = []
    for h in range(2):
        for i, ref in enumerate((k_hbm, v_hbm)):
            for n, (g, dst) in enumerate(((o, kv.at[c, h, i]), (1 - o, other.at[h, i]))):
                src = ref.at[pl.ds(h * half, half), head_cols(2 * tp + g, HEAD_DIM)]
                loads.append(pltpu.make_async_copy(src, dst, load_sem.at[4 * h + 2 * i + n]))
    for load in loads:
        load.start()
    load_q = pltpu.make_async_copy(q_hbm.at[:, head_cols(o, span)], q_raw.at[1], load_sem.at[8])
    load_q.start()

    barrier = pltpu.get_barrier_semaphore()
    beside = 2 * (chip + 1 - 2 * lax.rem(chip, 2))
    across = 2 * lax.rem(chip + 2, 4)
    for target in (partner, beside, beside + 1, across, across + 1):
        pl.semaphore_signal(barrier, inc=1, device_id={"ctx": target})
    v_t[...] = jnp.ones(v_t.shape, bf16)
    pl.semaphore_wait(barrier, 5)

    def remote(src, dst, send, recv, target):
        return pltpu.make_async_remote_copy(
            src_ref=src, dst_ref=dst, send_sem=send, recv_sem=recv, device_id={"ctx": target})

    def piece(b, h, send, target):
        return remote(kv.at[b, h], kv.at[b, h], send, recv_sem.at[b, h], target)

    give_q = remote(q_hbm.at[:, head_cols(1 - o, span)], q_raw.at[0], pair_sem.at[0], pair_sem.at[1], partner)
    give_kv = remote(other, kv.at[c], pair_sem.at[2], pair_sem.at[3], partner)
    give_q.start()
    for load in loads:
        load.wait()
    sends = []
    for n, (wanted, base, flip) in enumerate((
            ((chip == 0) | (chip == 2), beside, 0), (chip < 2, across, 1))):
        for k, (h, swap) in enumerate(((0, 0), (0, 1), (1, 0), (1, 1))):
            sem = send_sem.at[n, k]
            same = piece(c, h, sem, base + o)
            cross = remote(other.at[h], kv.at[c, h], sem, recv_sem.at[c, h], base + 1 - o)
            if flip:
                first, then = (same, cross), (cross, same)
                sends.append((wanted & (chip == 1), first[swap]))
                sends.append((wanted & (chip == 0), then[swap]))
            else:
                sends.append((wanted, (same, cross)[swap]))
    for wanted, copy in sends:
        pl.when(wanted)(copy.start)
    give_kv.start()

    def prepare(slot):
        for h in range(shared):
            x = q_raw[slot, :, h * HEAD_DIM:(h + 1) * HEAD_DIM].astype(f32) * EXP2_SCALE
            x = x.T
            top = x.astype(bf16)
            low = (x - top.astype(f32)).astype(bf16)
            for s in range(2):
                cols = slice(s * half, (s + 1) * half)
                q_t[slot * shared + h, s, :HEAD_DIM] = top[:, cols]
                q_t[slot * shared + h, s, HEAD_DIM:] = low[:, cols]

    def turn(slot, b1, h1, b2, h2):
        for s, (b, h) in enumerate(((b1, h1), (b2, h2))):
            v_t[slot, s, :HEAD_DIM] = kv[b, h, 1].astype(f32).T.astype(bf16)

    def bands(x):
        return x.reshape(x.shape[0] // 8, 8, rows)

    def pipeline(*accs):
        accs = iter(accs)
        s_acc = [[[next(accs) for _ in range(2)] for _ in range(2)] for _ in range(2)]
        o_acc = [[[next(accs) for _ in range(2)] for _ in range(2)] for _ in range(2)]

        def unit(i):
            return i % 2, i // 2 % 2

        def score(i, t, keys):
            m, d = unit(i)
            q = jnp.concatenate([q_t[t, 0], q_t[t, 1]], 1)
            pltpu.matmul_push_rhs(q, staging_register=0, mxu_index=m)
            for s, (b, h) in enumerate(keys):
                k = kv[b, h, 0]
                pltpu.matmul_acc_lhs(s_acc[m][d][s], jnp.concatenate([k, k], 1),
                                     load_staged_rhs=None if s else 0)

        def collect(i, t, masked, first):
            m, d = unit(i)
            top = None
            for s in range(2):
                x = pltpu.matmul_pop(s_acc[m][d][s])
                if masked:
                    key = lax.broadcasted_iota(jnp.int32, x.shape, 0) + s * half
                    row = lax.broadcasted_iota(jnp.int32, x.shape, 1)
                    x = jnp.where(key <= row, x, MASKED)
                ring[i % RING, s * half:(s + 1) * half] = x
                most = jnp.max(bands(x), 0)
                top = most if top is None else jnp.maximum(top, most)
            top = jnp.broadcast_to(jnp.max(top, 0, keepdims=True), (8, rows))
            if not first:
                before = peak[t]
                top = jnp.maximum(before, top)
                shrink[t] = jnp.exp2(before - top)
            peak[t] = top

        def weigh(i, t, slot):
            m, d = unit(i)
            p = jnp.exp2(bands(ring[i % RING]) - peak[t][None]).reshape(rows, rows).astype(bf16)
            v = jnp.concatenate([v_t[slot, 0], v_t[slot, 1]], 1)
            pltpu.matmul_push_rhs(p, staging_register=1, mxu_index=m)
            pltpu.matmul_acc_lhs(o_acc[m][d][0], v[:HEAD_DIM], load_staged_rhs=1)
            pltpu.matmul_acc_lhs(o_acc[m][d][1], v[HEAD_DIM:])

        def add(i, t, first):
            m, d = unit(i)
            new = pltpu.matmul_pop(o_acc[m][d][0])
            total = pltpu.matmul_pop(o_acc[m][d][1])[:8]
            if not first:
                scale = shrink[t]
                new = (bands(acc[t, :HEAD_DIM]) * scale[None]).reshape(HEAD_DIM, rows) + new
                total = acc[t, HEAD_DIM:] * scale + total
            acc[t, :HEAD_DIM] = new
            acc[t, HEAD_DIM:] = total

        pairs = lambda b: ((b, 0), (b, 1))
        late = o * shared
        jobs = []
        for h in range(shared):
            jobs.append((shared + h, pairs(c), 0, True, True))
        for h in range(shared):
            jobs.append((h, pairs(partner), 1, True, True))
        for h in range(shared):
            jobs.append((late + h, pairs(2 * chip), o, False, False))

        load_q.wait()
        prepare(1)
        turn(0, c, 0, c, 1)

        def meet():
            give_kv.wait_recv()
            give_q.wait_recv()
            prepare(0)
            turn(1, partner, 0, partner, 1)

        def start(i):
            if i == shared:
                meet()
            score(i, jobs[i][0], jobs[i][1])

        count = len(jobs)
        for i in range(AHEAD):
            start(i)
        for j in range(count + LAG + HOLD):
            k = j - LAG
            if 0 <= k - HOLD:
                add(k - HOLD, jobs[k - HOLD][0], jobs[k - HOLD][4])
            if 0 <= k < count:
                weigh(k, jobs[k][0], jobs[k][2])
            if j < count:
                collect(j, jobs[j][0], jobs[j][3], jobs[j][4])
            if j + AHEAD < count:
                start(j + AHEAD)

        for t in range(tiles - LAG - HOLD, tiles):
            shrink[t] = jnp.ones((8, rows), f32)
        for t in range(tiles - LAG, tiles):
            ring[t % RING] = jnp.full((rows, rows), MASKED, f32)

        def plan(r):
            e = lax.rem(r + o, 2)
            early = r < lax.select(chip == 3, 4, 2)
            b1 = lax.select(chip == 1, o, lax.select(chip == 2, lax.select(early, 1 - o, 2),
                                                     lax.select(early, 2 + e, 0)))
            b2 = lax.select(chip == 1, 1 - o, lax.select(chip == 2, lax.select(early, o, 3),
                                                         lax.select(early, 4 + e, 1)))
            h = lax.select(chip == 3, lax.select(early, r // 2, r - 4), lax.rem(r, 2))
            target = 2 * lax.select(chip == 3, 2, 3) + o
            return b1, b2, h, early, piece(b1, h, relay_sem.at[r], target)

        def sweep(r, carry):
            b1, b2, h, early, onward = plan(r)
            onward.wait_recv()
            pl.when(early)(onward.start)
            piece(b2, h, relay_sem.at[r], partner).wait_recv()
            slot = lax.rem(r, 2)
            turn(slot, b1, h, b2, h)
            keys = ((b1, h), (b2, h))
            for i in range(AHEAD):
                score(i, i, keys)
            for j in range(tiles):
                k = (j - LAG) % tiles
                n = (j - LAG - HOLD) % tiles
                add(n, n, False)
                weigh(k, k, slot if j >= LAG else 1 - slot)
                collect(j, j, False, False)
                if j + AHEAD < tiles:
                    score(j + AHEAD, j + AHEAD, keys)
            return carry

        rounds = 2 * chip
        lax.fori_loop(0, rounds, sweep, 0)

        def result(t):
            scale = 1.0 / acc[t, HEAD_DIM:]
            x = (bands(acc[t, :HEAD_DIM]) * scale[None]).reshape(HEAD_DIM, rows)
            return x.T.astype(o_ref.dtype)

        def give(h):
            cols = head_cols(o * shared + h, HEAD_DIM)
            return remote(stage.at[h], o_ref.at[:, cols], out_sem.at[0, h], out_sem.at[1, h], partner)

        def take(h):
            cols = head_cols((1 - o) * shared + h, HEAD_DIM)
            return remote(stage.at[h], o_ref.at[:, cols], out_sem.at[0, h], out_sem.at[1, h], partner)

        last = lax.rem(rounds + 1, 2)
        for k in range(tiles - LAG, tiles):
            weigh(k, k, last)
            add(k - HOLD, k - HOLD, False)
        for h in range(shared):
            stage[h] = result(h)
            if h >= 2:
                give(h - 2).start()
        for k in range(tiles - HOLD, tiles):
            add(k, k, False)
        for h in range(shared):
            cols = head_cols(o * shared + h, HEAD_DIM)
            o_ref[:, cols] = result(shared + h)
            if h < 2:
                give(shared - 2 + h).start()

        def drain(r, carry):
            _, _, _, early, onward = plan(r)
            pl.when(early)(onward.wait_send)
            return carry

        lax.fori_loop(0, rounds, drain, 0)
        for h in range(shared):
            take(h).wait_recv()
        for h in range(shared):
            give(h).wait_send()
        for wanted, copy in sends:
            pl.when(wanted)(copy.wait_send)
        give_q.wait_send()
        give_kv.wait_send()

    specs = [pltpu.ACC(m)((half, rows), f32) for m in range(2) for _ in range(4)]
    specs += [pltpu.ACC(m)((n, rows), f32) for m in range(2) for _ in range(2) for n in (HEAD_DIM, SUMS)]
    pl.run_scoped(pipeline, *specs)


def paired(rows, width, shared):
    half, tiles = rows // 2, 2 * shared
    bf16, f32, dma = jnp.bfloat16, jnp.float32, pltpu.SemaphoreType.DMA
    return pl.pallas_call(
        functools.partial(paired_kernel, shared),
        out_shape=pltpu.VMEM((rows, width), bf16),
        in_specs=[pl.BlockSpec(memory_space=pltpu.HBM)] * 3,
        out_specs=pl.BlockSpec(memory_space=pltpu.VMEM),
        scratch_shapes=[
            pltpu.VMEM((2, rows, shared * HEAD_DIM), bf16),
            pltpu.VMEM((tiles, 2, 2 * HEAD_DIM, half), bf16),
            pltpu.VMEM((8, 2, 2, half, HEAD_DIM), bf16),
            pltpu.VMEM((2, 2, half, HEAD_DIM), bf16),
            pltpu.VMEM((tiles, HEAD_DIM + 8, rows), f32),
            pltpu.VMEM((tiles, 8, rows), f32),
            pltpu.VMEM((tiles, 8, rows), f32),
            pltpu.VMEM((RING, rows, rows), f32),
            pltpu.VMEM((2, 2, HEAD_DIM + SUMS, half), bf16),
            pltpu.VMEM((shared, rows, HEAD_DIM), bf16),
            dma((9,)), dma((4,)), dma((2, 4)), dma((6,)), dma((8, 2)), dma((2, shared)),
        ],
        compiler_params=pltpu.CompilerParams(
            collective_id=1, has_side_effects=True, vmem_limit_bytes=60 * 1024 * 1024))


def solution(mesh):
    nc = mesh.shape["ctx"]

    def step(queries, keys, values):
        rows, width = queries.shape
        per_dev = width // HEAD_DIM
        group = HEADS // KV_HEADS
        kv_dev = per_dev // min(group, per_dev)
        if nc == 8 and kv_dev == 2 and rows == 2 * HEAD_DIM and per_dev == 2 * group:
            return paired(rows, width, group)(queries, keys, values)
        any_space = pl.BlockSpec(memory_space=pltpu.HBM)
        return pl.pallas_call(
            functools.partial(kernel, nc, per_dev, group, kv_dev),
            out_shape=pltpu.VMEM((rows, width), jnp.bfloat16),
            in_specs=[any_space] * 3,
            out_specs=pl.BlockSpec(memory_space=pltpu.VMEM),
            scratch_shapes=[
                pltpu.VMEM((rows, width), jnp.bfloat16),
                pltpu.VMEM((nc, kv_dev, 2, rows, HEAD_DIM), jnp.bfloat16),
                pltpu.VMEM((per_dev, rows, 2 * LANES), jnp.float32),
                pltpu.VMEM((per_dev, rows, LANES), jnp.float32),
                pltpu.SemaphoreType.DMA((2 * kv_dev + 1,)),
                pltpu.SemaphoreType.DMA((nc // 2, kv_dev)),
                pltpu.SemaphoreType.DMA((nc // 2, kv_dev)),
                pltpu.SemaphoreType.DMA((nc // 2, kv_dev)),
                pltpu.SemaphoreType.DMA((nc, kv_dev)),
            ],
            compiler_params=pltpu.CompilerParams(
                collective_id=0, has_side_effects=True, vmem_limit_bytes=60 * 1024 * 1024),
        )(queries, keys, values)

    return jax.shard_map(
        step, mesh=mesh,
        in_specs=(P("ctx", "tp"), P("ctx", None), P("ctx", None)),
        out_specs=P("ctx", "tp"), check_vma=False)
```

```python
import functools
import math

import jax
import jax.numpy as jnp
from jax import lax
from jax.experimental import pallas as pl
from jax.experimental.pallas import tpu as pltpu
from jax.sharding import PartitionSpec as P

HEADS = 64
KV_HEADS = 8
HEAD_DIM = 128
LANES = 128
MASKED = -1e30
CHUNK = 8
DEPTH = 1
ROUTED = 1
EXP2_SCALE = HEAD_DIM ** -0.5 * math.log2(math.e)


def attend_heads(q_v, kv, acc, peak, heads, kv_head, blocks, masked, first):
    k = jnp.concatenate([kv[b, kv_head, 0] for b in blocks], 0)
    v = jnp.concatenate([kv[b, kv_head, 1] for b in blocks], 0)
    v = jnp.concatenate([v, jnp.ones((v.shape[0], LANES), v.dtype)], 1)
    rows, count = q_v.shape[0], k.shape[0]

    def score(h):
        q = q_v[:, pl.ds(pl.multiple_of(h * HEAD_DIM, HEAD_DIM), HEAD_DIM)]
        return lax.dot_general(q, k, (((1,), (1,)), ((), ())), preferred_element_type=jnp.float32)

    def fold(h, s):
        if masked:
            row = lax.broadcasted_iota(jnp.int32, s.shape, 0)
            col = lax.broadcasted_iota(jnp.int32, s.shape, 1)
            s = jnp.where(col <= row, s, MASKED)
        top = jnp.broadcast_to(jnp.max(s, axis=1, keepdims=True), (rows, LANES))
        if not first:
            before = peak[h]
            top = jnp.maximum(before, top)
        peak[h] = top
        wide = jnp.concatenate([top] * (count // LANES), 1)
        w = jnp.exp2((s - wide) * EXP2_SCALE).astype(jnp.bfloat16)
        new = jnp.dot(w, v, preferred_element_type=jnp.float32)
        if not first:
            shrink = jnp.exp2((before - top) * EXP2_SCALE)
            new = acc[h] * jnp.concatenate([shrink, shrink], 1) + new
        acc[h] = new

    ahead = [score(h) for h in heads[:DEPTH]]
    for i, h in enumerate(heads):
        if i + DEPTH < len(heads):
            ahead.append(score(heads[i + DEPTH]))
        fold(h, ahead.pop(0))


def kernel(nc, per_dev, group, kv_dev, q_hbm, k_hbm, v_hbm, o_ref,
           q_v, kv, acc, peak, loc_sem, send_sem, fwd_sem, far_sem, recv_sem):
    c = lax.axis_index("ctx")
    tp = lax.axis_index("tp")
    odd = lax.rem(c, 2)
    pair = c // 2
    partner = c + 1 - 2 * odd
    shared = per_dev // kv_dev
    chunk = min(CHUNK, shared)
    square = nc == 8 and kv_dev == 2
    base = tp * per_dev // group

    loads = []
    for g in range(kv_dev):
        cols = pl.ds(pl.multiple_of((base + g) * HEAD_DIM, HEAD_DIM), HEAD_DIM)
        loads.append([
            pltpu.make_async_copy(ref.at[:, cols], kv.at[c, g, i], loc_sem.at[2 * g + i])
            for i, ref in enumerate((k_hbm, v_hbm))])
        for load in loads[g]:
            load.start()
    load_q = pltpu.make_async_copy(q_hbm, q_v, loc_sem.at[2 * kv_dev])
    load_q.start()

    barrier = pltpu.get_barrier_semaphore()
    pl.semaphore_signal(barrier, inc=1, device_id={"ctx": partner})
    for i in range(1, nc // 2):
        pl.semaphore_signal(barrier, inc=1, device_id={"ctx": lax.rem(c + 2 * i, nc)})
    pl.semaphore_wait(barrier, nc // 2)

    def copy_to(b, g, target, sem):
        return pltpu.make_async_remote_copy(
            src_ref=kv.at[b, g], dst_ref=kv.at[b, g], send_sem=sem, recv_sem=recv_sem.at[b, g],
            device_id={"ctx": target})

    for load in sum(loads, []):
        load.wait()
    sends, late = [], []
    for g in range(kv_dev):
        sends.append((odd == 0, copy_to(c, g, partner, send_sem.at[0, g])))
        if square:
            beside = copy_to(c, g, lax.rem(c + 2, nc), send_sem.at[1, g])
            sends.append((lax.rem(pair, 2) == 0, beside))
            if g >= ROUTED:
                late.append(beside)
            first = kv_dev - 1 - g
            other = lax.select(pair == 0, first, g)
            sends.append((pair < 2, copy_to(c, other, lax.rem(c + 4, nc), send_sem.at[2, g])))
        else:
            for i in range(1, nc // 2):
                sends.append((c + 2 * i < nc, copy_to(c, g, lax.rem(c + 2 * i, nc), send_sem.at[i, g])))
    for wanted, copy in sends:
        pl.when(wanted)(copy.start)
    load_q.wait()

    def item(t):
        if not square:
            return pair - 1 - t // kv_dev, lax.rem(t, kv_dev)
        third = (lax.select(t < 4, 2 - lax.rem(t, 2), 0), lax.select(t < 4, t // 2, t - 4))
        second = (t // 2, lax.rem((t + 1) // 2 + 1, 2))
        return (lax.select(pair == 3, third[0], lax.select(pair == 2, second[0], 0)),
                lax.select(pair == 3, third[1], lax.select(pair == 2, second[1], t)))

    def onward(p, g):
        mine = 2 * p + odd
        up = ((pair == 1) & (g == 0)) | ((pair == 2) & (p == 0) & (g == 1))
        back = (pair == 3) & (p == 1) & (g < ROUTED)
        target = lax.select(pair == 3, 4 + odd, 6 + odd)
        return up | back, copy_to(mine, g, target, far_sem.at[p, g])

    def pull(t):
        p, g = item(t)
        copy = copy_to(2 * p + odd, g, partner, fwd_sem.at[p, g])
        copy.wait_recv()
        if square:
            wanted, far = onward(p, g)
            pl.when(wanted)(far.start)
        copy.start()

    def sweep(blocks, kv_head, masked, first):
        def body(n, carry):
            heads = [n * chunk + i for i in range(chunk)]
            g = n * chunk // shared if kv_head is None else kv_head
            attend_heads(q_v, kv, acc, peak, heads, g, blocks, masked, first)
            return carry
        return body

    def finish(g, carry):
        for i in range(shared):
            h = g * shared + i
            out = acc[h, :, :LANES] / acc[h, :, LANES:]
            o_ref[:, pl.ds(pl.multiple_of(h * HEAD_DIM, HEAD_DIM), HEAD_DIM)] = out.astype(o_ref.dtype)
        return carry

    chunks = per_dev // chunk
    steps = pair * kv_dev
    lax.fori_loop(0, chunks, sweep([c], None, True, True), 0)

    if square:
        for copy in late:
            pl.when(pair == 1)(copy.start)

    def first_pulls():
        pull(0)
        if square:
            pl.when(pair == 3)(functools.partial(pull, 1))

    @pl.when(odd == 1)
    def _():
        for g in range(kv_dev):
            copy_to(c - 1, g, partner, send_sem.at[0, g]).wait_recv()
        work = sweep([c - 1], None, False, False)

        def body(n, carry):
            pl.when((n == chunks // 2) & (pair > 0))(first_pulls)
            return work(n, carry)

        lax.fori_loop(0, chunks, body, 0)

    pl.when((odd == 0) & (pair > 0))(first_pulls)

    def step(t, carry):
        p, g = item(t)
        copy_to(2 * p + 1 - odd, g, partner, fwd_sem.at[p, g]).wait_recv()
        body = sweep([2 * p, 2 * p + 1], g, False, False)

        done = (pair == 3) & (t == 0) if square else False

        @pl.when((t + 1 < steps) & jnp.logical_not(done))
        def _():
            pull(t + 1)

        per_head = shared // chunk
        lax.fori_loop(g * per_head, (g + 1) * per_head, body, 0)

        @pl.when(t >= steps - kv_dev)
        def _():
            finish(g, 0)
        return carry

    lax.fori_loop(0, steps, step, 0)

    @pl.when(pair == 0)
    def _():
        lax.fori_loop(0, kv_dev, finish, 0)

    def drain(t, carry):
        p, g = item(t)
        copy_to(2 * p + odd, g, partner, fwd_sem.at[p, g]).wait_send()
        if square:
            wanted, far = onward(p, g)
            pl.when(wanted)(far.wait_send)
        return carry

    lax.fori_loop(0, steps, drain, 0)
    for wanted, copy in sends:
        pl.when(wanted)(copy.wait_send)
    for copy in late:
        pl.when(pair == 1)(copy.wait_send)


AHEAD = 4
LAG = 4
HOLD = 2
RING = 8
SUMS = 16
PARTS = 2


def paired_kernel(shared, q_hbm, k_hbm, v_hbm, o_ref, q_raw, q_t, kv, other, acc, peak, shrink,
                  ring, v_t, stage, load_sem, pair_sem, send_sem, relay_sem, recv_sem, out_sem):
    c = lax.axis_index("ctx")
    tp = lax.axis_index("tp")
    o = lax.rem(c, 2)
    chip = c // 2
    partner = c + 1 - 2 * o
    rows = q_raw.shape[1]
    half = rows // 2
    span = shared * HEAD_DIM
    tiles = 2 * shared
    f32, bf16 = jnp.float32, jnp.bfloat16

    def head_cols(g, width):
        return pl.ds(pl.multiple_of(g * width, width), width)

    loads = []
    for h in range(2):
        for i, ref in enumerate((k_hbm, v_hbm)):
            for n, (g, dst) in enumerate(((o, kv.at[c, h, i]), (1 - o, other.at[h, i]))):
                src = ref.at[pl.ds(h * half, half), head_cols(2 * tp + g, HEAD_DIM)]
                loads.append(pltpu.make_async_copy(src, dst, load_sem.at[4 * h + 2 * i + n]))
    for load in loads:
        load.start()
    load_q = pltpu.make_async_copy(q_hbm.at[:, head_cols(o, span)], q_raw.at[1], load_sem.at[8])
    load_q.start()

    barrier = pltpu.get_barrier_semaphore()
    beside = 2 * (chip + 1 - 2 * lax.rem(chip, 2))
    across = 2 * lax.rem(chip + 2, 4)
    for target in (partner, beside, beside + 1, across, across + 1):
        pl.semaphore_signal(barrier, inc=1, device_id={"ctx": target})
    v_t[...] = jnp.ones(v_t.shape, bf16)
    pl.semaphore_wait(barrier, 5)

    def remote(src, dst, send, recv, target):
        return pltpu.make_async_remote_copy(
            src_ref=src, dst_ref=dst, send_sem=send, recv_sem=recv, device_id={"ctx": target})

    def piece(b, h, send, target):
        return remote(kv.at[b, h], kv.at[b, h], send, recv_sem.at[b, h], target)

    give_q = remote(q_hbm.at[:, head_cols(1 - o, span)], q_raw.at[0], pair_sem.at[0], pair_sem.at[1], partner)
    give_kv = remote(other, kv.at[c], pair_sem.at[2], pair_sem.at[3], partner)
    give_q.start()
    for load in loads:
        load.wait()
    sends = []
    for n, (wanted, base, flip) in enumerate((
            ((chip == 0) | (chip == 2), beside, 0), (chip < 2, across, 1))):
        for k, (h, swap) in enumerate(((0, 0), (0, 1), (1, 0), (1, 1))):
            sem = send_sem.at[n, k]
            same = piece(c, h, sem, base + o)
            cross = remote(other.at[h], kv.at[c, h], sem, recv_sem.at[c, h], base + 1 - o)
            if flip:
                first, then = (same, cross), (cross, same)
                sends.append((wanted & (chip == 1), first[swap]))
                sends.append((wanted & (chip == 0), then[swap]))
            else:
                sends.append((wanted, (same, cross)[swap]))
    for wanted, copy in sends:
        pl.when(wanted)(copy.start)
    give_kv.start()

    def prepare(slot):
        for h in range(shared):
            x = q_raw[slot, :, h * HEAD_DIM:(h + 1) * HEAD_DIM].astype(f32) * EXP2_SCALE
            x = x.T
            top = x.astype(bf16)
            low = (x - top.astype(f32)).astype(bf16)
            for s in range(2):
                cols = slice(s * half, (s + 1) * half)
                q_t[slot * shared + h, s, :HEAD_DIM] = top[:, cols]
                q_t[slot * shared + h, s, HEAD_DIM:] = low[:, cols]

    def turn(slot, b1, h1, b2, h2):
        for s, (b, h) in enumerate(((b1, h1), (b2, h2))):
            v_t[slot, s, :HEAD_DIM] = kv[b, h, 1].astype(f32).T.astype(bf16)

    def bands(x):
        return x.reshape(x.shape[0] // 8, 8, rows)

    def pipeline(*accs):
        accs = iter(accs)
        s_acc = [[[next(accs) for _ in range(2)] for _ in range(2)] for _ in range(2)]
        o_acc = [[[next(accs) for _ in range(2)] for _ in range(2)] for _ in range(2)]

        def unit(i):
            return i % 2, i // 2 % 2

        def score(i, t, keys):
            m, d = unit(i)
            q = jnp.concatenate([q_t[t, 0], q_t[t, 1]], 1)
            pltpu.matmul_push_rhs(q, staging_register=0, mxu_index=m)
            for s, (b, h) in enumerate(keys):
                k = kv[b, h, 0]
                pltpu.matmul_acc_lhs(s_acc[m][d][s], jnp.concatenate([k, k], 1),
                                     load_staged_rhs=None if s else 0)

        def collect(i, t, masked, first):
            m, d = unit(i)
            top = None
            for s in range(2):
                x = pltpu.matmul_pop(s_acc[m][d][s])
                if masked:
                    key = lax.broadcasted_iota(jnp.int32, x.shape, 0) + s * half
                    row = lax.broadcasted_iota(jnp.int32, x.shape, 1)
                    x = jnp.where(key <= row, x, MASKED)
                ring[i % RING, s * half:(s + 1) * half] = x
                most = jnp.max(bands(x), 0)
                top = most if top is None else jnp.maximum(top, most)
            top = jnp.broadcast_to(jnp.max(top, 0, keepdims=True), (8, rows))
            if not first:
                before = peak[t]
                top = jnp.maximum(before, top)
                shrink[t] = jnp.exp2(before - top)
            peak[t] = top

        def weigh(i, t, slot):
            m, d = unit(i)
            p = jnp.exp2(bands(ring[i % RING]) - peak[t][None]).reshape(rows, rows).astype(bf16)
            v = jnp.concatenate([v_t[slot, 0], v_t[slot, 1]], 1)
            pltpu.matmul_push_rhs(p, staging_register=1, mxu_index=m)
            pltpu.matmul_acc_lhs(o_acc[m][d][0], v[:HEAD_DIM], load_staged_rhs=1)
            pltpu.matmul_acc_lhs(o_acc[m][d][1], v[HEAD_DIM:])

        def add(i, t, first):
            m, d = unit(i)
            new = pltpu.matmul_pop(o_acc[m][d][0])
            total = pltpu.matmul_pop(o_acc[m][d][1])[:8]
            if not first:
                scale = shrink[t]
                new = (bands(acc[t, :HEAD_DIM]) * scale[None]).reshape(HEAD_DIM, rows) + new
                total = acc[t, HEAD_DIM:] * scale + total
            acc[t, :HEAD_DIM] = new
            acc[t, HEAD_DIM:] = total

        pairs = lambda b: ((b, 0), (b, 1))
        late = o * shared
        jobs = []
        for h in range(shared):
            jobs.append((shared + h, pairs(c), 0, True, True))
        for h in range(shared):
            jobs.append((h, pairs(partner), 1, True, True))
        for h in range(shared):
            jobs.append((late + h, pairs(2 * chip), o, False, False))

        load_q.wait()
        prepare(1)
        turn(0, c, 0, c, 1)

        def meet():
            give_kv.wait_recv()
            give_q.wait_recv()
            prepare(0)
            turn(1, partner, 0, partner, 1)

        def start(i):
            if i == shared:
                meet()
            score(i, jobs[i][0], jobs[i][1])

        count = len(jobs)
        for i in range(AHEAD):
            start(i)
        for j in range(count + LAG + HOLD):
            k = j - LAG
            if 0 <= k - HOLD:
                add(k - HOLD, jobs[k - HOLD][0], jobs[k - HOLD][4])
            if 0 <= k < count:
                weigh(k, jobs[k][0], jobs[k][2])
            if j < count:
                collect(j, jobs[j][0], jobs[j][3], jobs[j][4])
            if j + AHEAD < count:
                start(j + AHEAD)

        for t in range(tiles - LAG - HOLD, tiles):
            shrink[t] = jnp.ones((8, rows), f32)
        for t in range(tiles - LAG, tiles):
            ring[t % RING] = jnp.full((rows, rows), MASKED, f32)

        def plan(r):
            e = lax.rem(r + o, 2)
            early = r < lax.select(chip == 3, 4, 2)
            b1 = lax.select(chip == 1, o, lax.select(chip == 2, lax.select(early, 1 - o, 2),
                                                     lax.select(early, 2 + e, 0)))
            b2 = lax.select(chip == 1, 1 - o, lax.select(chip == 2, lax.select(early, o, 3),
                                                         lax.select(early, 4 + e, 1)))
            h = lax.select(chip == 3, lax.select(early, r // 2, r - 4), lax.rem(r, 2))
            target = 2 * lax.select(chip == 3, 2, 3) + o
            return b1, b2, h, early, piece(b1, h, relay_sem.at[r], target)

        def result(t):
            scale = 1.0 / acc[t, HEAD_DIM:]
            x = (bands(acc[t, :HEAD_DIM]) * scale[None]).reshape(HEAD_DIM, rows)
            return x.T.astype(o_ref.dtype)

        def set_aside(h):
            stage[:, h * HEAD_DIM:(h + 1) * HEAD_DIM] = result(h)

        def keep(h):
            o_ref[:, head_cols(o * shared + h, HEAD_DIM)] = result(shared + h)

        part = shared // PARTS

        def give(n, g):
            cols = head_cols(g * PARTS + n, part * HEAD_DIM)
            src = stage.at[:, n * part * HEAD_DIM:(n + 1) * part * HEAD_DIM]
            return remote(src, o_ref.at[:, cols], out_sem.at[0, n], out_sem.at[1, n], partner)

        def sweep(r, final):
            b1, b2, h, early, onward = plan(r)
            onward.wait_recv()
            pl.when(early)(onward.start)
            piece(b2, h, relay_sem.at[r], partner).wait_recv()
            slot = lax.rem(r, 2)
            turn(slot, b1, h, b2, h)
            keys = ((b1, h), (b2, h))
            for i in range(AHEAD):
                score(i, i, keys)
            for j in range(tiles):
                k = (j - LAG) % tiles
                n = (j - LAG - HOLD) % tiles
                add(n, n, False)
                weigh(k, k, slot if j >= LAG else 1 - slot)
                collect(j, j, False, False)
                if j + AHEAD < tiles:
                    score(j + AHEAD, j + AHEAD, keys)
                if final and j >= LAG + HOLD:
                    if n < shared:
                        set_aside(n)
                    else:
                        keep(n - shared)
                    if 0 < n <= shared and n % part == 0:
                        give(n // part - 1, o).start()

        rounds = 2 * chip

        def body(r, carry):
            sweep(r, False)
            return carry

        @pl.when(chip > 0)
        def _():
            lax.fori_loop(0, rounds - 1, body, 0)
            sweep(rounds - 1, True)

        @pl.when(chip == 0)
        def _():
            for h in range(shared):
                set_aside(h)
            for h in range(tiles - LAG - HOLD - shared):
                keep(h)
            for n in range(PARTS):
                give(n, o).start()

        last = lax.rem(rounds + 1, 2)
        for k in range(tiles - LAG, tiles):
            weigh(k, k, last)
            add(k - HOLD, k - HOLD, False)
            keep(k - HOLD - shared)
        for k in range(tiles - HOLD, tiles):
            add(k, k, False)
            keep(k - shared)

        def drain(r, carry):
            _, _, _, early, onward = plan(r)
            pl.when(early)(onward.wait_send)
            return carry

        lax.fori_loop(0, rounds, drain, 0)
        for n in range(PARTS):
            give(n, 1 - o).wait_recv()
            give(n, o).wait_send()
        for wanted, copy in sends:
            pl.when(wanted)(copy.wait_send)
        give_q.wait_send()
        give_kv.wait_send()

    specs = [pltpu.ACC(m)((half, rows), f32) for m in range(2) for _ in range(4)]
    specs += [pltpu.ACC(m)((n, rows), f32) for m in range(2) for _ in range(2) for n in (HEAD_DIM, SUMS)]
    pl.run_scoped(pipeline, *specs)


def paired(rows, width, shared):
    half, tiles = rows // 2, 2 * shared
    bf16, f32, dma = jnp.bfloat16, jnp.float32, pltpu.SemaphoreType.DMA
    return pl.pallas_call(
        functools.partial(paired_kernel, shared),
        out_shape=pltpu.VMEM((rows, width), bf16),
        in_specs=[pl.BlockSpec(memory_space=pltpu.HBM)] * 3,
        out_specs=pl.BlockSpec(memory_space=pltpu.VMEM),
        scratch_shapes=[
            pltpu.VMEM((2, rows, shared * HEAD_DIM), bf16),
            pltpu.VMEM((tiles, 2, 2 * HEAD_DIM, half), bf16),
            pltpu.VMEM((8, 2, 2, half, HEAD_DIM), bf16),
            pltpu.VMEM((2, 2, half, HEAD_DIM), bf16),
            pltpu.VMEM((tiles, HEAD_DIM + 8, rows), f32),
            pltpu.VMEM((tiles, 8, rows), f32),
            pltpu.VMEM((tiles, 8, rows), f32),
            pltpu.VMEM((RING, rows, rows), f32),
            pltpu.VMEM((2, 2, HEAD_DIM + SUMS, half), bf16),
            pltpu.VMEM((rows, shared * HEAD_DIM), bf16),
            dma((9,)), dma((4,)), dma((2, 4)), dma((6,)), dma((8, 2)), dma((2, PARTS)),
        ],
        compiler_params=pltpu.CompilerParams(
            collective_id=1, has_side_effects=True, vmem_limit_bytes=60 * 1024 * 1024))


def solution(mesh):
    nc = mesh.shape["ctx"]

    def step(queries, keys, values):
        rows, width = queries.shape
        per_dev = width // HEAD_DIM
        group = HEADS // KV_HEADS
        kv_dev = per_dev // min(group, per_dev)
        if nc == 8 and kv_dev == 2 and rows == 2 * HEAD_DIM and per_dev == 2 * group:
            return paired(rows, width, group)(queries, keys, values)
        any_space = pl.BlockSpec(memory_space=pltpu.HBM)
        return pl.pallas_call(
            functools.partial(kernel, nc, per_dev, group, kv_dev),
            out_shape=pltpu.VMEM((rows, width), jnp.bfloat16),
            in_specs=[any_space] * 3,
            out_specs=pl.BlockSpec(memory_space=pltpu.VMEM),
            scratch_shapes=[
                pltpu.VMEM((rows, width), jnp.bfloat16),
                pltpu.VMEM((nc, kv_dev, 2, rows, HEAD_DIM), jnp.bfloat16),
                pltpu.VMEM((per_dev, rows, 2 * LANES), jnp.float32),
                pltpu.VMEM((per_dev, rows, LANES), jnp.float32),
                pltpu.SemaphoreType.DMA((2 * kv_dev + 1,)),
                pltpu.SemaphoreType.DMA((nc // 2, kv_dev)),
                pltpu.SemaphoreType.DMA((nc // 2, kv_dev)),
                pltpu.SemaphoreType.DMA((nc // 2, kv_dev)),
                pltpu.SemaphoreType.DMA((nc, kv_dev)),
            ],
            compiler_params=pltpu.CompilerParams(
                collective_id=0, has_side_effects=True, vmem_limit_bytes=60 * 1024 * 1024),
        )(queries, keys, values)

    return jax.shard_map(
        step, mesh=mesh,
        in_specs=(P("ctx", "tp"), P("ctx", None), P("ctx", None)),
        out_specs=P("ctx", "tp"), check_vma=False)
```

```python
import functools
import math

import jax
import jax.numpy as jnp
from jax import lax
from jax.experimental import pallas as pl
from jax.experimental.pallas import tpu as pltpu
from jax.sharding import PartitionSpec as P

HEADS = 64
KV_HEADS = 8
HEAD_DIM = 128
LANES = 128
MASKED = -1e30
CHUNK = 8
DEPTH = 1
ROUTED = 1
EXP2_SCALE = HEAD_DIM ** -0.5 * math.log2(math.e)


def attend_heads(q_v, kv, acc, peak, heads, kv_head, blocks, masked, first):
    k = jnp.concatenate([kv[b, kv_head, 0] for b in blocks], 0)
    v = jnp.concatenate([kv[b, kv_head, 1] for b in blocks], 0)
    v = jnp.concatenate([v, jnp.ones((v.shape[0], LANES), v.dtype)], 1)
    rows, count = q_v.shape[0], k.shape[0]

    def score(h):
        q = q_v[:, pl.ds(pl.multiple_of(h * HEAD_DIM, HEAD_DIM), HEAD_DIM)]
        return lax.dot_general(q, k, (((1,), (1,)), ((), ())), preferred_element_type=jnp.float32)

    def fold(h, s):
        if masked:
            row = lax.broadcasted_iota(jnp.int32, s.shape, 0)
            col = lax.broadcasted_iota(jnp.int32, s.shape, 1)
            s = jnp.where(col <= row, s, MASKED)
        top = jnp.broadcast_to(jnp.max(s, axis=1, keepdims=True), (rows, LANES))
        if not first:
            before = peak[h]
            top = jnp.maximum(before, top)
        peak[h] = top
        wide = jnp.concatenate([top] * (count // LANES), 1)
        w = jnp.exp2((s - wide) * EXP2_SCALE).astype(jnp.bfloat16)
        new = jnp.dot(w, v, preferred_element_type=jnp.float32)
        if not first:
            shrink = jnp.exp2((before - top) * EXP2_SCALE)
            new = acc[h] * jnp.concatenate([shrink, shrink], 1) + new
        acc[h] = new

    ahead = [score(h) for h in heads[:DEPTH]]
    for i, h in enumerate(heads):
        if i + DEPTH < len(heads):
            ahead.append(score(heads[i + DEPTH]))
        fold(h, ahead.pop(0))


def kernel(nc, per_dev, group, kv_dev, q_hbm, k_hbm, v_hbm, o_ref,
           q_v, kv, acc, peak, loc_sem, send_sem, fwd_sem, far_sem, recv_sem):
    c = lax.axis_index("ctx")
    tp = lax.axis_index("tp")
    odd = lax.rem(c, 2)
    pair = c // 2
    partner = c + 1 - 2 * odd
    shared = per_dev // kv_dev
    chunk = min(CHUNK, shared)
    square = nc == 8 and kv_dev == 2
    base = tp * per_dev // group

    loads = []
    for g in range(kv_dev):
        cols = pl.ds(pl.multiple_of((base + g) * HEAD_DIM, HEAD_DIM), HEAD_DIM)
        loads.append([
            pltpu.make_async_copy(ref.at[:, cols], kv.at[c, g, i], loc_sem.at[2 * g + i])
            for i, ref in enumerate((k_hbm, v_hbm))])
        for load in loads[g]:
            load.start()
    load_q = pltpu.make_async_copy(q_hbm, q_v, loc_sem.at[2 * kv_dev])
    load_q.start()

    barrier = pltpu.get_barrier_semaphore()
    pl.semaphore_signal(barrier, inc=1, device_id={"ctx": partner})
    for i in range(1, nc // 2):
        pl.semaphore_signal(barrier, inc=1, device_id={"ctx": lax.rem(c + 2 * i, nc)})
    pl.semaphore_wait(barrier, nc // 2)

    def copy_to(b, g, target, sem):
        return pltpu.make_async_remote_copy(
            src_ref=kv.at[b, g], dst_ref=kv.at[b, g], send_sem=sem, recv_sem=recv_sem.at[b, g],
            device_id={"ctx": target})

    for load in sum(loads, []):
        load.wait()
    sends, late = [], []
    for g in range(kv_dev):
        sends.append((odd == 0, copy_to(c, g, partner, send_sem.at[0, g])))
        if square:
            beside = copy_to(c, g, lax.rem(c + 2, nc), send_sem.at[1, g])
            sends.append((lax.rem(pair, 2) == 0, beside))
            if g >= ROUTED:
                late.append(beside)
            first = kv_dev - 1 - g
            other = lax.select(pair == 0, first, g)
            sends.append((pair < 2, copy_to(c, other, lax.rem(c + 4, nc), send_sem.at[2, g])))
        else:
            for i in range(1, nc // 2):
                sends.append((c + 2 * i < nc, copy_to(c, g, lax.rem(c + 2 * i, nc), send_sem.at[i, g])))
    for wanted, copy in sends:
        pl.when(wanted)(copy.start)
    load_q.wait()

    def item(t):
        if not square:
            return pair - 1 - t // kv_dev, lax.rem(t, kv_dev)
        third = (lax.select(t < 4, 2 - lax.rem(t, 2), 0), lax.select(t < 4, t // 2, t - 4))
        second = (t // 2, lax.rem((t + 1) // 2 + 1, 2))
        return (lax.select(pair == 3, third[0], lax.select(pair == 2, second[0], 0)),
                lax.select(pair == 3, third[1], lax.select(pair == 2, second[1], t)))

    def onward(p, g):
        mine = 2 * p + odd
        up = ((pair == 1) & (g == 0)) | ((pair == 2) & (p == 0) & (g == 1))
        back = (pair == 3) & (p == 1) & (g < ROUTED)
        target = lax.select(pair == 3, 4 + odd, 6 + odd)
        return up | back, copy_to(mine, g, target, far_sem.at[p, g])

    def pull(t):
        p, g = item(t)
        copy = copy_to(2 * p + odd, g, partner, fwd_sem.at[p, g])
        copy.wait_recv()
        if square:
            wanted, far = onward(p, g)
            pl.when(wanted)(far.start)
        copy.start()

    def sweep(blocks, kv_head, masked, first):
        def body(n, carry):
            heads = [n * chunk + i for i in range(chunk)]
            g = n * chunk // shared if kv_head is None else kv_head
            attend_heads(q_v, kv, acc, peak, heads, g, blocks, masked, first)
            return carry
        return body

    def finish(g, carry):
        for i in range(shared):
            h = g * shared + i
            out = acc[h, :, :LANES] / acc[h, :, LANES:]
            o_ref[:, pl.ds(pl.multiple_of(h * HEAD_DIM, HEAD_DIM), HEAD_DIM)] = out.astype(o_ref.dtype)
        return carry

    chunks = per_dev // chunk
    steps = pair * kv_dev
    lax.fori_loop(0, chunks, sweep([c], None, True, True), 0)

    if square:
        for copy in late:
            pl.when(pair == 1)(copy.start)

    def first_pulls():
        pull(0)
        if square:
            pl.when(pair == 3)(functools.partial(pull, 1))

    @pl.when(odd == 1)
    def _():
        for g in range(kv_dev):
            copy_to(c - 1, g, partner, send_sem.at[0, g]).wait_recv()
        work = sweep([c - 1], None, False, False)

        def body(n, carry):
            pl.when((n == chunks // 2) & (pair > 0))(first_pulls)
            return work(n, carry)

        lax.fori_loop(0, chunks, body, 0)

    pl.when((odd == 0) & (pair > 0))(first_pulls)

    def step(t, carry):
        p, g = item(t)
        copy_to(2 * p + 1 - odd, g, partner, fwd_sem.at[p, g]).wait_recv()
        body = sweep([2 * p, 2 * p + 1], g, False, False)

        done = (pair == 3) & (t == 0) if square else False

        @pl.when((t + 1 < steps) & jnp.logical_not(done))
        def _():
            pull(t + 1)

        per_head = shared // chunk
        lax.fori_loop(g * per_head, (g + 1) * per_head, body, 0)

        @pl.when(t >= steps - kv_dev)
        def _():
            finish(g, 0)
        return carry

    lax.fori_loop(0, steps, step, 0)

    @pl.when(pair == 0)
    def _():
        lax.fori_loop(0, kv_dev, finish, 0)

    def drain(t, carry):
        p, g = item(t)
        copy_to(2 * p + odd, g, partner, fwd_sem.at[p, g]).wait_send()
        if square:
            wanted, far = onward(p, g)
            pl.when(wanted)(far.wait_send)
        return carry

    lax.fori_loop(0, steps, drain, 0)
    for wanted, copy in sends:
        pl.when(wanted)(copy.wait_send)
    for copy in late:
        pl.when(pair == 1)(copy.wait_send)


AHEAD = 4
LAG = 4
HOLD = 2
RING = 8
SUMS = 16
PARTS = 2
LATE = 2


def paired_kernel(shared, q_hbm, k_hbm, v_hbm, o_ref, q_raw, q_t, kv, other, acc, peak, shrink,
                  ring, v_t, stage, load_sem, pair_sem, send_sem, relay_sem, recv_sem, out_sem):
    c = lax.axis_index("ctx")
    tp = lax.axis_index("tp")
    o = lax.rem(c, 2)
    chip = c // 2
    partner = c + 1 - 2 * o
    rows = q_raw.shape[1]
    half = rows // 2
    span = shared * HEAD_DIM
    tiles = 2 * shared
    f32, bf16 = jnp.float32, jnp.bfloat16

    def head_cols(g, width):
        return pl.ds(pl.multiple_of(g * width, width), width)

    loads = []
    for h in range(2):
        for i, ref in enumerate((k_hbm, v_hbm)):
            for n, (g, dst) in enumerate(((o, kv.at[c, h, i]), (1 - o, other.at[h, i]))):
                src = ref.at[pl.ds(h * half, half), head_cols(2 * tp + g, HEAD_DIM)]
                loads.append(pltpu.make_async_copy(src, dst, load_sem.at[4 * h + 2 * i + n]))
    for load in loads:
        load.start()
    load_q = pltpu.make_async_copy(q_hbm.at[:, head_cols(o, span)], q_raw.at[1], load_sem.at[8])
    load_q.start()

    barrier = pltpu.get_barrier_semaphore()
    beside = 2 * (chip + 1 - 2 * lax.rem(chip, 2))
    across = 2 * lax.rem(chip + 2, 4)
    for target in (partner, beside, beside + 1, across, across + 1):
        pl.semaphore_signal(barrier, inc=1, device_id={"ctx": target})
    middle = (chip == 1) | (chip == 2)
    opposite = 2 * (3 - chip)

    @pl.when(middle)
    def _():
        for target in (opposite, opposite + 1):
            pl.semaphore_signal(barrier, inc=1, device_id={"ctx": target})

    v_t[...] = jnp.ones(v_t.shape, bf16)
    pl.semaphore_wait(barrier, lax.select(middle, 7, 5))

    def remote(src, dst, send, recv, target):
        return pltpu.make_async_remote_copy(
            src_ref=src, dst_ref=dst, send_sem=send, recv_sem=recv, device_id={"ctx": target})

    def piece(b, h, send, target):
        return remote(kv.at[b, h], kv.at[b, h], send, recv_sem.at[b, h], target)

    give_q = remote(q_hbm.at[:, head_cols(1 - o, span)], q_raw.at[0], pair_sem.at[0], pair_sem.at[1], partner)
    give_kv = remote(other, kv.at[c], pair_sem.at[2], pair_sem.at[3], partner)
    give_q.start()
    for load in loads:
        load.wait()
    sends = []
    for n, (wanted, base, flip) in enumerate((
            ((chip == 0) | (chip == 2), beside, 0), (chip < 2, across, 1))):
        for k, (h, swap) in enumerate(((0, 0), (0, 1), (1, 0), (1, 1))):
            sem = send_sem.at[n, k]
            same = piece(c, h, sem, base + o)
            cross = remote(other.at[h], kv.at[c, h], sem, recv_sem.at[c, h], base + 1 - o)
            if flip:
                first, then = (same, cross), (cross, same)
                sends.append((wanted & (chip == 1), first[swap]))
                sends.append((wanted & (chip == 0), then[swap]))
            else:
                sends.append((wanted, (same, cross)[swap]))
    for wanted, copy in sends:
        pl.when(wanted)(copy.start)
    give_kv.start()
    late = [remote(other.at[1], kv.at[c, 1], send_sem.at[2, 1], recv_sem.at[c, 1], opposite + 1 - o)]
    sends += [(chip == 1, copy) for copy in late]

    def send_late():
        for copy in late:
            pl.when(chip == 1)(copy.start)

    if LATE == 0:
        send_late()

    def prepare(slot):
        for h in range(shared):
            x = q_raw[slot, :, h * HEAD_DIM:(h + 1) * HEAD_DIM].astype(f32) * EXP2_SCALE
            x = x.T
            top = x.astype(bf16)
            low = (x - top.astype(f32)).astype(bf16)
            for s in range(2):
                cols = slice(s * half, (s + 1) * half)
                q_t[slot * shared + h, s, :HEAD_DIM] = top[:, cols]
                q_t[slot * shared + h, s, HEAD_DIM:] = low[:, cols]

    def turn(slot, b1, h1, b2, h2):
        for s, (b, h) in enumerate(((b1, h1), (b2, h2))):
            v_t[slot, s, :HEAD_DIM] = kv[b, h, 1].astype(f32).T.astype(bf16)

    def bands(x):
        return x.reshape(x.shape[0] // 8, 8, rows)

    def pipeline(*accs):
        accs = iter(accs)
        s_acc = [[[next(accs) for _ in range(2)] for _ in range(2)] for _ in range(2)]
        o_acc = [[[next(accs) for _ in range(2)] for _ in range(2)] for _ in range(2)]

        def unit(i):
            return i % 2, i // 2 % 2

        def score(i, t, keys):
            m, d = unit(i)
            q = jnp.concatenate([q_t[t, 0], q_t[t, 1]], 1)
            pltpu.matmul_push_rhs(q, staging_register=0, mxu_index=m)
            for s, (b, h) in enumerate(keys):
                k = kv[b, h, 0]
                pltpu.matmul_acc_lhs(s_acc[m][d][s], jnp.concatenate([k, k], 1),
                                     load_staged_rhs=None if s else 0)

        def collect(i, t, masked, first):
            m, d = unit(i)
            top = None
            for s in range(2):
                x = pltpu.matmul_pop(s_acc[m][d][s])
                if masked:
                    key = lax.broadcasted_iota(jnp.int32, x.shape, 0) + s * half
                    row = lax.broadcasted_iota(jnp.int32, x.shape, 1)
                    x = jnp.where(key <= row, x, MASKED)
                ring[i % RING, s * half:(s + 1) * half] = x
                most = jnp.max(bands(x), 0)
                top = most if top is None else jnp.maximum(top, most)
            top = jnp.broadcast_to(jnp.max(top, 0, keepdims=True), (8, rows))
            if not first:
                before = peak[t]
                top = jnp.maximum(before, top)
                shrink[t] = jnp.exp2(before - top)
            peak[t] = top

        def weigh(i, t, slot):
            m, d = unit(i)
            p = jnp.exp2(bands(ring[i % RING]) - peak[t][None]).reshape(rows, rows).astype(bf16)
            v = jnp.concatenate([v_t[slot, 0], v_t[slot, 1]], 1)
            pltpu.matmul_push_rhs(p, staging_register=1, mxu_index=m)
            pltpu.matmul_acc_lhs(o_acc[m][d][0], v[:HEAD_DIM], load_staged_rhs=1)
            pltpu.matmul_acc_lhs(o_acc[m][d][1], v[HEAD_DIM:])

        def add(i, t, first):
            m, d = unit(i)
            new = pltpu.matmul_pop(o_acc[m][d][0])
            total = pltpu.matmul_pop(o_acc[m][d][1])[:8]
            if not first:
                scale = shrink[t]
                new = (bands(acc[t, :HEAD_DIM]) * scale[None]).reshape(HEAD_DIM, rows) + new
                total = acc[t, HEAD_DIM:] * scale + total
            acc[t, :HEAD_DIM] = new
            acc[t, HEAD_DIM:] = total

        pairs = lambda b: ((b, 0), (b, 1))
        lower = o * shared
        jobs = []
        for h in range(shared):
            jobs.append((shared + h, pairs(c), 0, True, True))
        for h in range(shared):
            jobs.append((h, pairs(partner), 1, True, True))
        for h in range(shared):
            jobs.append((lower + h, pairs(2 * chip), o, False, False))

        load_q.wait()
        prepare(1)
        turn(0, c, 0, c, 1)

        def meet():
            if LATE == 1:
                send_late()
            give_kv.wait_recv()
            give_q.wait_recv()
            prepare(0)
            turn(1, partner, 0, partner, 1)

        def start(i):
            if i == shared:
                meet()
            score(i, jobs[i][0], jobs[i][1])

        count = len(jobs)
        for i in range(AHEAD):
            start(i)
        for j in range(count + LAG + HOLD):
            k = j - LAG
            if 0 <= k - HOLD:
                add(k - HOLD, jobs[k - HOLD][0], jobs[k - HOLD][4])
            if 0 <= k < count:
                weigh(k, jobs[k][0], jobs[k][2])
            if j < count:
                collect(j, jobs[j][0], jobs[j][3], jobs[j][4])
            if j + AHEAD < count:
                start(j + AHEAD)

        for t in range(tiles - LAG - HOLD, tiles):
            shrink[t] = jnp.ones((8, rows), f32)
        for t in range(tiles - LAG, tiles):
            ring[t % RING] = jnp.full((rows, rows), MASKED, f32)

        def plan(r):
            e = lax.rem(r + o, 2)
            early = r < lax.select(chip == 3, 4, 2)
            b1 = lax.select(chip == 1, o, lax.select(chip == 2, lax.select(early, 1 - o, 2),
                                                     lax.select(early, 2 + e, 0)))
            b2 = lax.select(chip == 1, 1 - o, lax.select(chip == 2, lax.select(early, o, 3),
                                                         lax.select(early, 4 + e, 1)))
            h = lax.select(chip == 3, lax.select(early, r // 2, r - 4), lax.rem(r, 2))
            target = 2 * lax.select(chip == 3, 2, 3) + o
            onward = early & (r < 3)
            return b1, b2, h, onward, piece(b1, h, relay_sem.at[r], target)

        def result(t):
            scale = 1.0 / acc[t, HEAD_DIM:]
            x = (bands(acc[t, :HEAD_DIM]) * scale[None]).reshape(HEAD_DIM, rows)
            return x.T.astype(o_ref.dtype)

        def set_aside(h):
            stage[:, h * HEAD_DIM:(h + 1) * HEAD_DIM] = result(h)

        def keep(h):
            o_ref[:, head_cols(o * shared + h, HEAD_DIM)] = result(shared + h)

        part = shared // PARTS

        def give(n, g):
            cols = head_cols(g * PARTS + n, part * HEAD_DIM)
            src = stage.at[:, n * part * HEAD_DIM:(n + 1) * part * HEAD_DIM]
            return remote(src, o_ref.at[:, cols], out_sem.at[0, n], out_sem.at[1, n], partner)

        def sweep(r, final):
            b1, b2, h, early, onward = plan(r)
            onward.wait_recv()
            pl.when(early)(onward.start)
            piece(b2, h, relay_sem.at[r], partner).wait_recv()
            slot = lax.rem(r, 2)
            turn(slot, b1, h, b2, h)
            keys = ((b1, h), (b2, h))
            for i in range(AHEAD):
                score(i, i, keys)
            for j in range(tiles):
                k = (j - LAG) % tiles
                n = (j - LAG - HOLD) % tiles
                add(n, n, False)
                weigh(k, k, slot if j >= LAG else 1 - slot)
                collect(j, j, False, False)
                if j + AHEAD < tiles:
                    score(j + AHEAD, j + AHEAD, keys)
                if final and j >= LAG + HOLD:
                    if n < shared:
                        set_aside(n)
                    else:
                        keep(n - shared)
                    if 0 < n <= shared and n % part == 0:
                        give(n // part - 1, o).start()

        if LATE == 2:
            send_late()
        rounds = 2 * chip

        def body(r, carry):
            sweep(r, False)
            return carry

        @pl.when(chip > 0)
        def _():
            lax.fori_loop(0, rounds - 1, body, 0)
            sweep(rounds - 1, True)

        @pl.when(chip == 0)
        def _():
            for h in range(shared):
                set_aside(h)
            for h in range(tiles - LAG - HOLD - shared):
                keep(h)
            for n in range(PARTS):
                give(n, o).start()

        last = lax.rem(rounds + 1, 2)
        for k in range(tiles - LAG, tiles):
            weigh(k, k, last)
            add(k - HOLD, k - HOLD, False)
            keep(k - HOLD - shared)
        for k in range(tiles - HOLD, tiles):
            add(k, k, False)
            keep(k - shared)

        def drain(r, carry):
            _, _, _, early, onward = plan(r)
            pl.when(early)(onward.wait_send)
            return carry

        lax.fori_loop(0, rounds, drain, 0)
        for n in range(PARTS):
            give(n, 1 - o).wait_recv()
            give(n, o).wait_send()
        for wanted, copy in sends:
            pl.when(wanted)(copy.wait_send)
        give_q.wait_send()
        give_kv.wait_send()

    specs = [pltpu.ACC(m)((half, rows), f32) for m in range(2) for _ in range(4)]
    specs += [pltpu.ACC(m)((n, rows), f32) for m in range(2) for _ in range(2) for n in (HEAD_DIM, SUMS)]
    pl.run_scoped(pipeline, *specs)


def paired(rows, width, shared):
    half, tiles = rows // 2, 2 * shared
    bf16, f32, dma = jnp.bfloat16, jnp.float32, pltpu.SemaphoreType.DMA
    return pl.pallas_call(
        functools.partial(paired_kernel, shared),
        out_shape=pltpu.VMEM((rows, width), bf16),
        in_specs=[pl.BlockSpec(memory_space=pltpu.HBM)] * 3,
        out_specs=pl.BlockSpec(memory_space=pltpu.VMEM),
        scratch_shapes=[
            pltpu.VMEM((2, rows, shared * HEAD_DIM), bf16),
            pltpu.VMEM((tiles, 2, 2 * HEAD_DIM, half), bf16),
            pltpu.VMEM((8, 2, 2, half, HEAD_DIM), bf16),
            pltpu.VMEM((2, 2, half, HEAD_DIM), bf16),
            pltpu.VMEM((tiles, HEAD_DIM + 8, rows), f32),
            pltpu.VMEM((tiles, 8, rows), f32),
            pltpu.VMEM((tiles, 8, rows), f32),
            pltpu.VMEM((RING, rows, rows), f32),
            pltpu.VMEM((2, 2, HEAD_DIM + SUMS, half), bf16),
            pltpu.VMEM((rows, shared * HEAD_DIM), bf16),
            dma((9,)), dma((4,)), dma((3, 4)), dma((6,)), dma((8, 2)), dma((2, PARTS)),
        ],
        compiler_params=pltpu.CompilerParams(
            collective_id=1, has_side_effects=True, vmem_limit_bytes=60 * 1024 * 1024))


def solution(mesh):
    nc = mesh.shape["ctx"]

    def step(queries, keys, values):
        rows, width = queries.shape
        per_dev = width // HEAD_DIM
        group = HEADS // KV_HEADS
        kv_dev = per_dev // min(group, per_dev)
        if nc == 8 and kv_dev == 2 and rows == 2 * HEAD_DIM and per_dev == 2 * group:
            return paired(rows, width, group)(queries, keys, values)
        any_space = pl.BlockSpec(memory_space=pltpu.HBM)
        return pl.pallas_call(
            functools.partial(kernel, nc, per_dev, group, kv_dev),
            out_shape=pltpu.VMEM((rows, width), jnp.bfloat16),
            in_specs=[any_space] * 3,
            out_specs=pl.BlockSpec(memory_space=pltpu.VMEM),
            scratch_shapes=[
                pltpu.VMEM((rows, width), jnp.bfloat16),
                pltpu.VMEM((nc, kv_dev, 2, rows, HEAD_DIM), jnp.bfloat16),
                pltpu.VMEM((per_dev, rows, 2 * LANES), jnp.float32),
                pltpu.VMEM((per_dev, rows, LANES), jnp.float32),
                pltpu.SemaphoreType.DMA((2 * kv_dev + 1,)),
                pltpu.SemaphoreType.DMA((nc // 2, kv_dev)),
                pltpu.SemaphoreType.DMA((nc // 2, kv_dev)),
                pltpu.SemaphoreType.DMA((nc // 2, kv_dev)),
                pltpu.SemaphoreType.DMA((nc, kv_dev)),
            ],
            compiler_params=pltpu.CompilerParams(
                collective_id=0, has_side_effects=True, vmem_limit_bytes=60 * 1024 * 1024),
        )(queries, keys, values)

    return jax.shard_map(
        step, mesh=mesh,
        in_specs=(P("ctx", "tp"), P("ctx", None), P("ctx", None)),
        out_specs=P("ctx", "tp"), check_vma=False)
```

```python
import functools
import math

import jax
import jax.numpy as jnp
from jax import lax
from jax.experimental import pallas as pl
from jax.experimental.pallas import tpu as pltpu
from jax.sharding import PartitionSpec as P

HEADS = 64
KV_HEADS = 8
HEAD_DIM = 128
LANES = 128
MASKED = -1e30
CHUNK = 8
DEPTH = 1
ROUTED = 1
EXP2_SCALE = HEAD_DIM ** -0.5 * math.log2(math.e)


def attend_heads(q_v, kv, acc, peak, heads, kv_head, blocks, masked, first):
    k = jnp.concatenate([kv[b, kv_head, 0] for b in blocks], 0)
    v = jnp.concatenate([kv[b, kv_head, 1] for b in blocks], 0)
    v = jnp.concatenate([v, jnp.ones((v.shape[0], LANES), v.dtype)], 1)
    rows, count = q_v.shape[0], k.shape[0]

    def score(h):
        q = q_v[:, pl.ds(pl.multiple_of(h * HEAD_DIM, HEAD_DIM), HEAD_DIM)]
        return lax.dot_general(q, k, (((1,), (1,)), ((), ())), preferred_element_type=jnp.float32)

    def fold(h, s):
        if masked:
            row = lax.broadcasted_iota(jnp.int32, s.shape, 0)
            col = lax.broadcasted_iota(jnp.int32, s.shape, 1)
            s = jnp.where(col <= row, s, MASKED)
        top = jnp.broadcast_to(jnp.max(s, axis=1, keepdims=True), (rows, LANES))
        if not first:
            before = peak[h]
            top = jnp.maximum(before, top)
        peak[h] = top
        wide = jnp.concatenate([top] * (count // LANES), 1)
        w = jnp.exp2((s - wide) * EXP2_SCALE).astype(jnp.bfloat16)
        new = jnp.dot(w, v, preferred_element_type=jnp.float32)
        if not first:
            shrink = jnp.exp2((before - top) * EXP2_SCALE)
            new = acc[h] * jnp.concatenate([shrink, shrink], 1) + new
        acc[h] = new

    ahead = [score(h) for h in heads[:DEPTH]]
    for i, h in enumerate(heads):
        if i + DEPTH < len(heads):
            ahead.append(score(heads[i + DEPTH]))
        fold(h, ahead.pop(0))


def kernel(nc, per_dev, group, kv_dev, q_hbm, k_hbm, v_hbm, o_ref,
           q_v, kv, acc, peak, loc_sem, send_sem, fwd_sem, far_sem, recv_sem):
    c = lax.axis_index("ctx")
    tp = lax.axis_index("tp")
    odd = lax.rem(c, 2)
    pair = c // 2
    partner = c + 1 - 2 * odd
    shared = per_dev // kv_dev
    chunk = min(CHUNK, shared)
    square = nc == 8 and kv_dev == 2
    base = tp * per_dev // group

    loads = []
    for g in range(kv_dev):
        cols = pl.ds(pl.multiple_of((base + g) * HEAD_DIM, HEAD_DIM), HEAD_DIM)
        loads.append([
            pltpu.make_async_copy(ref.at[:, cols], kv.at[c, g, i], loc_sem.at[2 * g + i])
            for i, ref in enumerate((k_hbm, v_hbm))])
        for load in loads[g]:
            load.start()
    load_q = pltpu.make_async_copy(q_hbm, q_v, loc_sem.at[2 * kv_dev])
    load_q.start()

    barrier = pltpu.get_barrier_semaphore()
    pl.semaphore_signal(barrier, inc=1, device_id={"ctx": partner})
    for i in range(1, nc // 2):
        pl.semaphore_signal(barrier, inc=1, device_id={"ctx": lax.rem(c + 2 * i, nc)})
    pl.semaphore_wait(barrier, nc // 2)

    def copy_to(b, g, target, sem):
        return pltpu.make_async_remote_copy(
            src_ref=kv.at[b, g], dst_ref=kv.at[b, g], send_sem=sem, recv_sem=recv_sem.at[b, g],
            device_id={"ctx": target})

    for load in sum(loads, []):
        load.wait()
    sends, late = [], []
    for g in range(kv_dev):
        sends.append((odd == 0, copy_to(c, g, partner, send_sem.at[0, g])))
        if square:
            beside = copy_to(c, g, lax.rem(c + 2, nc), send_sem.at[1, g])
            sends.append((lax.rem(pair, 2) == 0, beside))
            if g >= ROUTED:
                late.append(beside)
            first = kv_dev - 1 - g
            other = lax.select(pair == 0, first, g)
            sends.append((pair < 2, copy_to(c, other, lax.rem(c + 4, nc), send_sem.at[2, g])))
        else:
            for i in range(1, nc // 2):
                sends.append((c + 2 * i < nc, copy_to(c, g, lax.rem(c + 2 * i, nc), send_sem.at[i, g])))
    for wanted, copy in sends:
        pl.when(wanted)(copy.start)
    load_q.wait()

    def item(t):
        if not square:
            return pair - 1 - t // kv_dev, lax.rem(t, kv_dev)
        third = (lax.select(t < 4, 2 - lax.rem(t, 2), 0), lax.select(t < 4, t // 2, t - 4))
        second = (t // 2, lax.rem((t + 1) // 2 + 1, 2))
        return (lax.select(pair == 3, third[0], lax.select(pair == 2, second[0], 0)),
                lax.select(pair == 3, third[1], lax.select(pair == 2, second[1], t)))

    def onward(p, g):
        mine = 2 * p + odd
        up = ((pair == 1) & (g == 0)) | ((pair == 2) & (p == 0) & (g == 1))
        back = (pair == 3) & (p == 1) & (g < ROUTED)
        target = lax.select(pair == 3, 4 + odd, 6 + odd)
        return up | back, copy_to(mine, g, target, far_sem.at[p, g])

    def pull(t):
        p, g = item(t)
        copy = copy_to(2 * p + odd, g, partner, fwd_sem.at[p, g])
        copy.wait_recv()
        if square:
            wanted, far = onward(p, g)
            pl.when(wanted)(far.start)
        copy.start()

    def sweep(blocks, kv_head, masked, first):
        def body(n, carry):
            heads = [n * chunk + i for i in range(chunk)]
            g = n * chunk // shared if kv_head is None else kv_head
            attend_heads(q_v, kv, acc, peak, heads, g, blocks, masked, first)
            return carry
        return body

    def finish(g, carry):
        for i in range(shared):
            h = g * shared + i
            out = acc[h, :, :LANES] / acc[h, :, LANES:]
            o_ref[:, pl.ds(pl.multiple_of(h * HEAD_DIM, HEAD_DIM), HEAD_DIM)] = out.astype(o_ref.dtype)
        return carry

    chunks = per_dev // chunk
    steps = pair * kv_dev
    lax.fori_loop(0, chunks, sweep([c], None, True, True), 0)

    if square:
        for copy in late:
            pl.when(pair == 1)(copy.start)

    def first_pulls():
        pull(0)
        if square:
            pl.when(pair == 3)(functools.partial(pull, 1))

    @pl.when(odd == 1)
    def _():
        for g in range(kv_dev):
            copy_to(c - 1, g, partner, send_sem.at[0, g]).wait_recv()
        work = sweep([c - 1], None, False, False)

        def body(n, carry):
            pl.when((n == chunks // 2) & (pair > 0))(first_pulls)
            return work(n, carry)

        lax.fori_loop(0, chunks, body, 0)

    pl.when((odd == 0) & (pair > 0))(first_pulls)

    def step(t, carry):
        p, g = item(t)
        copy_to(2 * p + 1 - odd, g, partner, fwd_sem.at[p, g]).wait_recv()
        body = sweep([2 * p, 2 * p + 1], g, False, False)

        done = (pair == 3) & (t == 0) if square else False

        @pl.when((t + 1 < steps) & jnp.logical_not(done))
        def _():
            pull(t + 1)

        per_head = shared // chunk
        lax.fori_loop(g * per_head, (g + 1) * per_head, body, 0)

        @pl.when(t >= steps - kv_dev)
        def _():
            finish(g, 0)
        return carry

    lax.fori_loop(0, steps, step, 0)

    @pl.when(pair == 0)
    def _():
        lax.fori_loop(0, kv_dev, finish, 0)

    def drain(t, carry):
        p, g = item(t)
        copy_to(2 * p + odd, g, partner, fwd_sem.at[p, g]).wait_send()
        if square:
            wanted, far = onward(p, g)
            pl.when(wanted)(far.wait_send)
        return carry

    lax.fori_loop(0, steps, drain, 0)
    for wanted, copy in sends:
        pl.when(wanted)(copy.wait_send)
    for copy in late:
        pl.when(pair == 1)(copy.wait_send)


AHEAD = 4
LAG = 3
HOLD = 2
RING = 8
SUMS = 16
ENDS = (4, 7, 8)


def paired_kernel(shared, q_hbm, k_hbm, v_hbm, o_ref, q_raw, q_t, kv, other, acc, peak, shrink,
                  ring, v_t, stage, load_sem, pair_sem, send_sem, relay_sem, recv_sem, out_sem):
    c = lax.axis_index("ctx")
    tp = lax.axis_index("tp")
    o = lax.rem(c, 2)
    chip = c // 2
    partner = c + 1 - 2 * o
    rows = q_raw.shape[1]
    half = rows // 2
    span = shared * HEAD_DIM
    tiles = 2 * shared
    f32, bf16 = jnp.float32, jnp.bfloat16

    def head_cols(g, width):
        return pl.ds(pl.multiple_of(g * width, width), width)

    loads = []
    for h in range(2):
        for i, ref in enumerate((k_hbm, v_hbm)):
            for n, (g, dst) in enumerate(((o, kv.at[c, h, i]), (1 - o, other.at[h, i]))):
                src = ref.at[pl.ds(h * half, half), head_cols(2 * tp + g, HEAD_DIM)]
                loads.append(pltpu.make_async_copy(src, dst, load_sem.at[4 * h + 2 * i + n]))
    for load in loads:
        load.start()
    load_q = pltpu.make_async_copy(q_hbm.at[:, head_cols(o, span)], q_raw.at[1], load_sem.at[8])
    load_q.start()

    barrier = pltpu.get_barrier_semaphore()
    beside = 2 * (chip + 1 - 2 * lax.rem(chip, 2))
    across = 2 * lax.rem(chip + 2, 4)
    for target in (partner, beside, beside + 1, across, across + 1):
        pl.semaphore_signal(barrier, inc=1, device_id={"ctx": target})
    middle = (chip == 1) | (chip == 2)
    opposite = 2 * (3 - chip)

    @pl.when(middle)
    def _():
        for target in (opposite, opposite + 1):
            pl.semaphore_signal(barrier, inc=1, device_id={"ctx": target})

    v_t[...] = jnp.ones(v_t.shape, bf16)
    pl.semaphore_wait(barrier, lax.select(middle, 7, 5))

    def remote(src, dst, send, recv, target):
        return pltpu.make_async_remote_copy(
            src_ref=src, dst_ref=dst, send_sem=send, recv_sem=recv, device_id={"ctx": target})

    def piece(b, h, send, target):
        return remote(kv.at[b, h], kv.at[b, h], send, recv_sem.at[b, h], target)

    give_q = remote(q_hbm.at[:, head_cols(1 - o, span)], q_raw.at[0], pair_sem.at[0], pair_sem.at[1], partner)
    give_kv = remote(other, kv.at[c], pair_sem.at[2], pair_sem.at[3], partner)
    give_q.start()
    for load in loads:
        load.wait()
    sends = []
    for n, (wanted, base, flip) in enumerate((
            ((chip == 0) | (chip == 2), beside, 0), (chip < 2, across, 1))):
        for k, (h, swap) in enumerate(((0, 0), (0, 1), (1, 0), (1, 1))):
            sem = send_sem.at[n, k]
            same = piece(c, h, sem, base + o)
            cross = remote(other.at[h], kv.at[c, h], sem, recv_sem.at[c, h], base + 1 - o)
            if flip:
                first, then = (same, cross), (cross, same)
                sends.append((wanted & (chip == 1), first[swap]))
                sends.append((wanted & (chip == 0), then[swap]))
            else:
                sends.append((wanted, (same, cross)[swap]))
    for wanted, copy in sends:
        pl.when(wanted)(copy.start)
    give_kv.start()
    late = [remote(other.at[1], kv.at[c, 1], send_sem.at[2, 1], recv_sem.at[c, 1], opposite + 1 - o)]
    sends += [(chip == 1, copy) for copy in late]

    def send_late():
        for copy in late:
            pl.when(chip == 1)(copy.start)

    def prepare(slot):
        for h in range(shared):
            x = q_raw[slot, :, h * HEAD_DIM:(h + 1) * HEAD_DIM].astype(f32) * EXP2_SCALE
            x = x.T
            top = x.astype(bf16)
            low = (x - top.astype(f32)).astype(bf16)
            for s in range(2):
                cols = slice(s * half, (s + 1) * half)
                q_t[slot * shared + h, s, :HEAD_DIM] = top[:, cols]
                q_t[slot * shared + h, s, HEAD_DIM:] = low[:, cols]

    def turn(slot, b1, h1, b2, h2):
        for s, (b, h) in enumerate(((b1, h1), (b2, h2))):
            v_t[slot, s, :HEAD_DIM] = kv[b, h, 1].astype(f32).T.astype(bf16)

    def bands(x):
        return x.reshape(x.shape[0] // 8, 8, rows)

    def pipeline(*accs):
        accs = iter(accs)
        s_acc = [[[next(accs) for _ in range(2)] for _ in range(2)] for _ in range(2)]
        o_acc = [[[next(accs) for _ in range(2)] for _ in range(2)] for _ in range(2)]

        def unit(i):
            return i % 2, i // 2 % 2

        def score(i, t, keys):
            m, d = unit(i)
            q = jnp.concatenate([q_t[t, 0], q_t[t, 1]], 1)
            pltpu.matmul_push_rhs(q, staging_register=0, mxu_index=m)
            for s, (b, h) in enumerate(keys):
                k = kv[b, h, 0]
                pltpu.matmul_acc_lhs(s_acc[m][d][s], jnp.concatenate([k, k], 1),
                                     load_staged_rhs=None if s else 0)

        def collect(i, t, masked, first):
            m, d = unit(i)
            top = None
            for s in range(2):
                x = pltpu.matmul_pop(s_acc[m][d][s])
                if masked:
                    key = lax.broadcasted_iota(jnp.int32, x.shape, 0) + s * half
                    row = lax.broadcasted_iota(jnp.int32, x.shape, 1)
                    x = jnp.where(key <= row, x, MASKED)
                ring[i % RING, s * half:(s + 1) * half] = x
                most = jnp.max(bands(x), 0)
                top = most if top is None else jnp.maximum(top, most)
            top = jnp.broadcast_to(jnp.max(top, 0, keepdims=True), (8, rows))
            if not first:
                before = peak[t]
                top = jnp.maximum(before, top)
                shrink[t] = jnp.exp2(before - top)
            peak[t] = top

        def weigh(i, t, slot):
            m, d = unit(i)
            p = jnp.exp2(bands(ring[i % RING]) - peak[t][None]).reshape(rows, rows).astype(bf16)
            v = jnp.concatenate([v_t[slot, 0], v_t[slot, 1]], 1)
            pltpu.matmul_push_rhs(p, staging_register=1, mxu_index=m)
            pltpu.matmul_acc_lhs(o_acc[m][d][0], v[:HEAD_DIM], load_staged_rhs=1)
            pltpu.matmul_acc_lhs(o_acc[m][d][1], v[HEAD_DIM:])

        def add(i, t, first):
            m, d = unit(i)
            new = pltpu.matmul_pop(o_acc[m][d][0])
            total = pltpu.matmul_pop(o_acc[m][d][1])[:8]
            if not first:
                scale = shrink[t]
                new = (bands(acc[t, :HEAD_DIM]) * scale[None]).reshape(HEAD_DIM, rows) + new
                total = acc[t, HEAD_DIM:] * scale + total
            acc[t, :HEAD_DIM] = new
            acc[t, HEAD_DIM:] = total

        pairs = lambda b: ((b, 0), (b, 1))
        lower = o * shared
        jobs = []
        for h in range(shared):
            jobs.append((shared + h, pairs(c), 0, True, True))
        for h in range(shared):
            jobs.append((h, pairs(partner), 1, True, True))
        for h in range(shared):
            jobs.append((lower + h, pairs(2 * chip), o, False, False))

        load_q.wait()
        prepare(1)
        turn(0, c, 0, c, 1)

        def meet():
            give_kv.wait_recv()
            give_q.wait_recv()
            prepare(0)
            turn(1, partner, 0, partner, 1)

        def start(i):
            if i == shared:
                meet()
            score(i, jobs[i][0], jobs[i][1])

        count = len(jobs)
        for i in range(AHEAD):
            start(i)
        for j in range(count + LAG + HOLD):
            k = j - LAG
            if 0 <= k - HOLD:
                add(k - HOLD, jobs[k - HOLD][0], jobs[k - HOLD][4])
            if 0 <= k < count:
                weigh(k, jobs[k][0], jobs[k][2])
            if j < count:
                collect(j, jobs[j][0], jobs[j][3], jobs[j][4])
            if j + AHEAD < count:
                start(j + AHEAD)

        for t in range(tiles - LAG - HOLD, tiles):
            shrink[t] = jnp.ones((8, rows), f32)
        for t in range(tiles - LAG, tiles):
            ring[t % RING] = jnp.full((rows, rows), MASKED, f32)

        def plan(r):
            e = lax.rem(r + o, 2)
            early = r < lax.select(chip == 3, 4, 2)
            b1 = lax.select(chip == 1, o, lax.select(chip == 2, lax.select(early, 1 - o, 2),
                                                     lax.select(early, 2 + e, 0)))
            b2 = lax.select(chip == 1, 1 - o, lax.select(chip == 2, lax.select(early, o, 3),
                                                         lax.select(early, 4 + e, 1)))
            h = lax.select(chip == 3, lax.select(early, r // 2, r - 4), lax.rem(r, 2))
            target = 2 * lax.select(chip == 3, 2, 3) + o
            onward = early & (r < 3)
            return b1, b2, h, onward, piece(b1, h, relay_sem.at[r], target)

        def result(t):
            scale = 1.0 / acc[t, HEAD_DIM:]
            x = (bands(acc[t, :HEAD_DIM]) * scale[None]).reshape(HEAD_DIM, rows)
            return x.T.astype(o_ref.dtype)

        def set_aside(h):
            stage[:, h * HEAD_DIM:(h + 1) * HEAD_DIM] = result(h)

        def keep(h):
            o_ref[:, head_cols(o * shared + h, HEAD_DIM)] = result(shared + h)

        ends = [shared * x // 8 for x in ENDS]
        begins = [0] + ends[:-1]

        def give(n, g):
            width = (ends[n] - begins[n]) * HEAD_DIM
            lo = begins[n] * HEAD_DIM
            cols = pl.ds(pl.multiple_of(g * span + lo, HEAD_DIM), width)
            src = stage.at[:, lo:lo + width]
            return remote(src, o_ref.at[:, cols], out_sem.at[0, n], out_sem.at[1, n], partner)

        def sweep(r, final):
            b1, b2, h, early, onward = plan(r)
            onward.wait_recv()
            pl.when(early)(onward.start)
            piece(b2, h, relay_sem.at[r], partner).wait_recv()
            slot = lax.rem(r, 2)
            turn(slot, b1, h, b2, h)
            keys = ((b1, h), (b2, h))
            for i in range(AHEAD):
                score(i, i, keys)
            for j in range(tiles):
                k = (j - LAG) % tiles
                n = (j - LAG - HOLD) % tiles
                add(n, n, False)
                weigh(k, k, slot if j >= LAG else 1 - slot)
                collect(j, j, False, False)
                if j + AHEAD < tiles:
                    score(j + AHEAD, j + AHEAD, keys)
                if final and j >= LAG + HOLD:
                    if n < shared:
                        set_aside(n)
                    else:
                        keep(n - shared)
                    if n + 1 in ends:
                        give(ends.index(n + 1), o).start()

        send_late()
        rounds = 2 * chip

        def body(r, carry):
            sweep(r, False)
            return carry

        @pl.when(chip > 0)
        def _():
            lax.fori_loop(0, rounds - 1, body, 0)
            sweep(rounds - 1, True)

        @pl.when(chip == 0)
        def _():
            for h in range(shared):
                set_aside(h)
            for h in range(tiles - LAG - HOLD - shared):
                keep(h)
            for n in range(len(ENDS)):
                give(n, o).start()

        last = lax.rem(rounds + 1, 2)
        for k in range(tiles - LAG, tiles):
            weigh(k, k, last)
            add(k - HOLD, k - HOLD, False)
            keep(k - HOLD - shared)
        for k in range(tiles - HOLD, tiles):
            add(k, k, False)
            keep(k - shared)

        def drain(r, carry):
            _, _, _, early, onward = plan(r)
            pl.when(early)(onward.wait_send)
            return carry

        lax.fori_loop(0, rounds, drain, 0)
        for n in range(len(ENDS)):
            give(n, 1 - o).wait_recv()
            give(n, o).wait_send()
        for wanted, copy in sends:
            pl.when(wanted)(copy.wait_send)
        give_q.wait_send()
        give_kv.wait_send()

    specs = [pltpu.ACC(m)((half, rows), f32) for m in range(2) for _ in range(4)]
    specs += [pltpu.ACC(m)((n, rows), f32) for m in range(2) for _ in range(2) for n in (HEAD_DIM, SUMS)]
    pl.run_scoped(pipeline, *specs)


def paired(rows, width, shared):
    half, tiles = rows // 2, 2 * shared
    bf16, f32, dma = jnp.bfloat16, jnp.float32, pltpu.SemaphoreType.DMA
    return pl.pallas_call(
        functools.partial(paired_kernel, shared),
        out_shape=pltpu.VMEM((rows, width), bf16),
        in_specs=[pl.BlockSpec(memory_space=pltpu.HBM)] * 3,
        out_specs=pl.BlockSpec(memory_space=pltpu.VMEM),
        scratch_shapes=[
            pltpu.VMEM((2, rows, shared * HEAD_DIM), bf16),
            pltpu.VMEM((tiles, 2, 2 * HEAD_DIM, half), bf16),
            pltpu.VMEM((8, 2, 2, half, HEAD_DIM), bf16),
            pltpu.VMEM((2, 2, half, HEAD_DIM), bf16),
            pltpu.VMEM((tiles, HEAD_DIM + 8, rows), f32),
            pltpu.VMEM((tiles, 8, rows), f32),
            pltpu.VMEM((tiles, 8, rows), f32),
            pltpu.VMEM((RING, rows, rows), f32),
            pltpu.VMEM((2, 2, HEAD_DIM + SUMS, half), bf16),
            pltpu.VMEM((rows, shared * HEAD_DIM), bf16),
            dma((9,)), dma((4,)), dma((3, 4)), dma((6,)), dma((8, 2)), dma((2, len(ENDS))),
        ],
        compiler_params=pltpu.CompilerParams(
            collective_id=1, has_side_effects=True, vmem_limit_bytes=60 * 1024 * 1024))


def solution(mesh):
    nc = mesh.shape["ctx"]

    def step(queries, keys, values):
        rows, width = queries.shape
        per_dev = width // HEAD_DIM
        group = HEADS // KV_HEADS
        kv_dev = per_dev // min(group, per_dev)
        if nc == 8 and kv_dev == 2 and rows == 2 * HEAD_DIM and per_dev == 2 * group:
            return paired(rows, width, group)(queries, keys, values)
        any_space = pl.BlockSpec(memory_space=pltpu.HBM)
        return pl.pallas_call(
            functools.partial(kernel, nc, per_dev, group, kv_dev),
            out_shape=pltpu.VMEM((rows, width), jnp.bfloat16),
            in_specs=[any_space] * 3,
            out_specs=pl.BlockSpec(memory_space=pltpu.VMEM),
            scratch_shapes=[
                pltpu.VMEM((rows, width), jnp.bfloat16),
                pltpu.VMEM((nc, kv_dev, 2, rows, HEAD_DIM), jnp.bfloat16),
                pltpu.VMEM((per_dev, rows, 2 * LANES), jnp.float32),
                pltpu.VMEM((per_dev, rows, LANES), jnp.float32),
                pltpu.SemaphoreType.DMA((2 * kv_dev + 1,)),
                pltpu.SemaphoreType.DMA((nc // 2, kv_dev)),
                pltpu.SemaphoreType.DMA((nc // 2, kv_dev)),
                pltpu.SemaphoreType.DMA((nc // 2, kv_dev)),
                pltpu.SemaphoreType.DMA((nc, kv_dev)),
            ],
            compiler_params=pltpu.CompilerParams(
                collective_id=0, has_side_effects=True, vmem_limit_bytes=60 * 1024 * 1024),
        )(queries, keys, values)

    return jax.shard_map(
        step, mesh=mesh,
        in_specs=(P("ctx", "tp"), P("ctx", None), P("ctx", None)),
        out_specs=P("ctx", "tp"), check_vma=False)
```

```python
import functools
import math

import jax
import jax.numpy as jnp
from jax import lax
from jax.experimental import pallas as pl
from jax.experimental.pallas import tpu as pltpu
from jax.sharding import PartitionSpec as P

HEADS = 64
KV_HEADS = 8
HEAD_DIM = 128
LANES = 128
MASKED = -1e30
CHUNK = 8
DEPTH = 1
ROUTED = 1
EXP2_SCALE = HEAD_DIM ** -0.5 * math.log2(math.e)


def attend_heads(q_v, kv, acc, peak, heads, kv_head, blocks, masked, first):
    k = jnp.concatenate([kv[b, kv_head, 0] for b in blocks], 0)
    v = jnp.concatenate([kv[b, kv_head, 1] for b in blocks], 0)
    v = jnp.concatenate([v, jnp.ones((v.shape[0], LANES), v.dtype)], 1)
    rows, count = q_v.shape[0], k.shape[0]

    def score(h):
        q = q_v[:, pl.ds(pl.multiple_of(h * HEAD_DIM, HEAD_DIM), HEAD_DIM)]
        return lax.dot_general(q, k, (((1,), (1,)), ((), ())), preferred_element_type=jnp.float32)

    def fold(h, s):
        if masked:
            row = lax.broadcasted_iota(jnp.int32, s.shape, 0)
            col = lax.broadcasted_iota(jnp.int32, s.shape, 1)
            s = jnp.where(col <= row, s, MASKED)
        top = jnp.broadcast_to(jnp.max(s, axis=1, keepdims=True), (rows, LANES))
        if not first:
            before = peak[h]
            top = jnp.maximum(before, top)
        peak[h] = top
        wide = jnp.concatenate([top] * (count // LANES), 1)
        w = jnp.exp2((s - wide) * EXP2_SCALE).astype(jnp.bfloat16)
        new = jnp.dot(w, v, preferred_element_type=jnp.float32)
        if not first:
            shrink = jnp.exp2((before - top) * EXP2_SCALE)
            new = acc[h] * jnp.concatenate([shrink, shrink], 1) + new
        acc[h] = new

    ahead = [score(h) for h in heads[:DEPTH]]
    for i, h in enumerate(heads):
        if i + DEPTH < len(heads):
            ahead.append(score(heads[i + DEPTH]))
        fold(h, ahead.pop(0))


def kernel(nc, per_dev, group, kv_dev, q_hbm, k_hbm, v_hbm, o_ref,
           q_v, kv, acc, peak, loc_sem, send_sem, fwd_sem, far_sem, recv_sem):
    c = lax.axis_index("ctx")
    tp = lax.axis_index("tp")
    odd = lax.rem(c, 2)
    pair = c // 2
    partner = c + 1 - 2 * odd
    shared = per_dev // kv_dev
    chunk = min(CHUNK, shared)
    square = nc == 8 and kv_dev == 2
    base = tp * per_dev // group

    loads = []
    for g in range(kv_dev):
        cols = pl.ds(pl.multiple_of((base + g) * HEAD_DIM, HEAD_DIM), HEAD_DIM)
        loads.append([
            pltpu.make_async_copy(ref.at[:, cols], kv.at[c, g, i], loc_sem.at[2 * g + i])
            for i, ref in enumerate((k_hbm, v_hbm))])
        for load in loads[g]:
            load.start()
    load_q = pltpu.make_async_copy(q_hbm, q_v, loc_sem.at[2 * kv_dev])
    load_q.start()

    barrier = pltpu.get_barrier_semaphore()
    pl.semaphore_signal(barrier, inc=1, device_id={"ctx": partner})
    for i in range(1, nc // 2):
        pl.semaphore_signal(barrier, inc=1, device_id={"ctx": lax.rem(c + 2 * i, nc)})
    pl.semaphore_wait(barrier, nc // 2)

    def copy_to(b, g, target, sem):
        return pltpu.make_async_remote_copy(
            src_ref=kv.at[b, g], dst_ref=kv.at[b, g], send_sem=sem, recv_sem=recv_sem.at[b, g],
            device_id={"ctx": target})

    for load in sum(loads, []):
        load.wait()
    sends, late = [], []
    for g in range(kv_dev):
        sends.append((odd == 0, copy_to(c, g, partner, send_sem.at[0, g])))
        if square:
            beside = copy_to(c, g, lax.rem(c + 2, nc), send_sem.at[1, g])
            sends.append((lax.rem(pair, 2) == 0, beside))
            if g >= ROUTED:
                late.append(beside)
            first = kv_dev - 1 - g
            other = lax.select(pair == 0, first, g)
            sends.append((pair < 2, copy_to(c, other, lax.rem(c + 4, nc), send_sem.at[2, g])))
        else:
            for i in range(1, nc // 2):
                sends.append((c + 2 * i < nc, copy_to(c, g, lax.rem(c + 2 * i, nc), send_sem.at[i, g])))
    for wanted, copy in sends:
        pl.when(wanted)(copy.start)
    load_q.wait()

    def item(t):
        if not square:
            return pair - 1 - t // kv_dev, lax.rem(t, kv_dev)
        third = (lax.select(t < 4, 2 - lax.rem(t, 2), 0), lax.select(t < 4, t // 2, t - 4))
        second = (t // 2, lax.rem((t + 1) // 2 + 1, 2))
        return (lax.select(pair == 3, third[0], lax.select(pair == 2, second[0], 0)),
                lax.select(pair == 3, third[1], lax.select(pair == 2, second[1], t)))

    def onward(p, g):
        mine = 2 * p + odd
        up = ((pair == 1) & (g == 0)) | ((pair == 2) & (p == 0) & (g == 1))
        back = (pair == 3) & (p == 1) & (g < ROUTED)
        target = lax.select(pair == 3, 4 + odd, 6 + odd)
        return up | back, copy_to(mine, g, target, far_sem.at[p, g])

    def pull(t):
        p, g = item(t)
        copy = copy_to(2 * p + odd, g, partner, fwd_sem.at[p, g])
        copy.wait_recv()
        if square:
            wanted, far = onward(p, g)
            pl.when(wanted)(far.start)
        copy.start()

    def sweep(blocks, kv_head, masked, first):
        def body(n, carry):
            heads = [n * chunk + i for i in range(chunk)]
            g = n * chunk // shared if kv_head is None else kv_head
            attend_heads(q_v, kv, acc, peak, heads, g, blocks, masked, first)
            return carry
        return body

    def finish(g, carry):
        for i in range(shared):
            h = g * shared + i
            out = acc[h, :, :LANES] / acc[h, :, LANES:]
            o_ref[:, pl.ds(pl.multiple_of(h * HEAD_DIM, HEAD_DIM), HEAD_DIM)] = out.astype(o_ref.dtype)
        return carry

    chunks = per_dev // chunk
    steps = pair * kv_dev
    lax.fori_loop(0, chunks, sweep([c], None, True, True), 0)

    if square:
        for copy in late:
            pl.when(pair == 1)(copy.start)

    def first_pulls():
        pull(0)
        if square:
            pl.when(pair == 3)(functools.partial(pull, 1))

    @pl.when(odd == 1)
    def _():
        for g in range(kv_dev):
            copy_to(c - 1, g, partner, send_sem.at[0, g]).wait_recv()
        work = sweep([c - 1], None, False, False)

        def body(n, carry):
            pl.when((n == chunks // 2) & (pair > 0))(first_pulls)
            return work(n, carry)

        lax.fori_loop(0, chunks, body, 0)

    pl.when((odd == 0) & (pair > 0))(first_pulls)

    def step(t, carry):
        p, g = item(t)
        copy_to(2 * p + 1 - odd, g, partner, fwd_sem.at[p, g]).wait_recv()
        body = sweep([2 * p, 2 * p + 1], g, False, False)

        done = (pair == 3) & (t == 0) if square else False

        @pl.when((t + 1 < steps) & jnp.logical_not(done))
        def _():
            pull(t + 1)

        per_head = shared // chunk
        lax.fori_loop(g * per_head, (g + 1) * per_head, body, 0)

        @pl.when(t >= steps - kv_dev)
        def _():
            finish(g, 0)
        return carry

    lax.fori_loop(0, steps, step, 0)

    @pl.when(pair == 0)
    def _():
        lax.fori_loop(0, kv_dev, finish, 0)

    def drain(t, carry):
        p, g = item(t)
        copy_to(2 * p + odd, g, partner, fwd_sem.at[p, g]).wait_send()
        if square:
            wanted, far = onward(p, g)
            pl.when(wanted)(far.wait_send)
        return carry

    lax.fori_loop(0, steps, drain, 0)
    for wanted, copy in sends:
        pl.when(wanted)(copy.wait_send)
    for copy in late:
        pl.when(pair == 1)(copy.wait_send)


AHEAD = 4
LAG = 3
HOLD = 2
RING = 8
SUMS = 16
ENDS = (4, 7, 8)


def paired_kernel(shared, q_hbm, k_hbm, v_hbm, o_ref, q_raw, q_t, kv, other, acc, peak, shrink,
                  ring, v_t, stage, load_sem, pair_sem, send_sem, relay_sem, recv_sem, out_sem):
    c = lax.axis_index("ctx")
    tp = lax.axis_index("tp")
    o = lax.rem(c, 2)
    chip = c // 2
    partner = c + 1 - 2 * o
    rows = q_raw.shape[1]
    half = rows // 2
    span = shared * HEAD_DIM
    tiles = 2 * shared
    f32, bf16 = jnp.float32, jnp.bfloat16

    def head_cols(g, width):
        return pl.ds(pl.multiple_of(g * width, width), width)

    loads = []
    for h in range(2):
        for i, ref in enumerate((k_hbm, v_hbm)):
            for n, (g, dst) in enumerate(((o, kv.at[c, h, i]), (1 - o, other.at[h, i]))):
                src = ref.at[pl.ds(h * half, half), head_cols(2 * tp + g, HEAD_DIM)]
                loads.append(pltpu.make_async_copy(src, dst, load_sem.at[4 * h + 2 * i + n]))
    barrier = pltpu.get_barrier_semaphore()
    beside = 2 * (chip + 1 - 2 * lax.rem(chip, 2))
    across = 2 * lax.rem(chip + 2, 4)
    for target in (partner, beside, beside + 1, across, across + 1):
        pl.semaphore_signal(barrier, inc=1, device_id={"ctx": target})
    middle = (chip == 1) | (chip == 2)
    opposite = 2 * (3 - chip)

    @pl.when(middle)
    def _():
        for target in (opposite, opposite + 1):
            pl.semaphore_signal(barrier, inc=1, device_id={"ctx": target})

    for load in loads:
        load.start()
    load_q = pltpu.make_async_copy(q_hbm.at[:, head_cols(o, span)], q_raw.at[1], load_sem.at[8])
    load_q.start()

    v_t[...] = jnp.ones(v_t.shape, bf16)
    pl.semaphore_wait(barrier, lax.select(middle, 7, 5))

    def remote(src, dst, send, recv, target):
        return pltpu.make_async_remote_copy(
            src_ref=src, dst_ref=dst, send_sem=send, recv_sem=recv, device_id={"ctx": target})

    def piece(b, h, send, target):
        return remote(kv.at[b, h], kv.at[b, h], send, recv_sem.at[b, h], target)

    give_q = remote(q_hbm.at[:, head_cols(1 - o, span)], q_raw.at[0], pair_sem.at[0], pair_sem.at[1], partner)
    give_kv = remote(other, kv.at[c], pair_sem.at[2], pair_sem.at[3], partner)
    for load in loads:
        load.wait()
    sends = []
    for n, (wanted, base, flip) in enumerate((
            ((chip == 0) | (chip == 2), beside, 0), (chip < 2, across, 1))):
        for k, (h, swap) in enumerate(((0, 0), (0, 1), (1, 0), (1, 1))):
            sem = send_sem.at[n, k]
            same = piece(c, h, sem, base + o)
            cross = remote(other.at[h], kv.at[c, h], sem, recv_sem.at[c, h], base + 1 - o)
            if flip:
                first, then = (same, cross), (cross, same)
                sends.append((wanted & (chip == 1), first[swap]))
                sends.append((wanted & (chip == 0), then[swap]))
            else:
                sends.append((wanted, (same, cross)[swap]))
    for wanted, copy in sends:
        pl.when(wanted)(copy.start)
    give_q.start()
    give_kv.start()
    late = [remote(other.at[1], kv.at[c, 1], send_sem.at[2, 1], recv_sem.at[c, 1], opposite + 1 - o)]
    sends += [(chip == 1, copy) for copy in late]

    def send_late():
        for copy in late:
            pl.when(chip == 1)(copy.start)

    def prepare(slot):
        for h in range(shared):
            x = q_raw[slot, :, h * HEAD_DIM:(h + 1) * HEAD_DIM].astype(f32) * EXP2_SCALE
            x = x.T
            top = x.astype(bf16)
            low = (x - top.astype(f32)).astype(bf16)
            for s in range(2):
                cols = slice(s * half, (s + 1) * half)
                q_t[slot * shared + h, s, :HEAD_DIM] = top[:, cols]
                q_t[slot * shared + h, s, HEAD_DIM:] = low[:, cols]

    def turn(slot, b1, h1, b2, h2):
        for s, (b, h) in enumerate(((b1, h1), (b2, h2))):
            v_t[slot, s, :HEAD_DIM] = kv[b, h, 1].astype(f32).T.astype(bf16)

    def bands(x):
        return x.reshape(x.shape[0] // 8, 8, rows)

    def pipeline(*accs):
        accs = iter(accs)
        s_acc = [[[next(accs) for _ in range(2)] for _ in range(2)] for _ in range(2)]
        o_acc = [[[next(accs) for _ in range(2)] for _ in range(2)] for _ in range(2)]

        def unit(i):
            return i % 2, i // 2 % 2

        def score(i, t, keys):
            m, d = unit(i)
            q = jnp.concatenate([q_t[t, 0], q_t[t, 1]], 1)
            pltpu.matmul_push_rhs(q, staging_register=0, mxu_index=m)
            for s, (b, h) in enumerate(keys):
                k = kv[b, h, 0]
                pltpu.matmul_acc_lhs(s_acc[m][d][s], jnp.concatenate([k, k], 1),
                                     load_staged_rhs=None if s else 0)

        def collect(i, t, masked, first):
            m, d = unit(i)
            top = None
            for s in range(2):
                x = pltpu.matmul_pop(s_acc[m][d][s])
                if masked:
                    key = lax.broadcasted_iota(jnp.int32, x.shape, 0) + s * half
                    row = lax.broadcasted_iota(jnp.int32, x.shape, 1)
                    x = jnp.where(key <= row, x, MASKED)
                ring[i % RING, s * half:(s + 1) * half] = x
                most = jnp.max(bands(x), 0)
                top = most if top is None else jnp.maximum(top, most)
            top = jnp.broadcast_to(jnp.max(top, 0, keepdims=True), (8, rows))
            if not first:
                before = peak[t]
                top = jnp.maximum(before, top)
                shrink[t] = jnp.exp2(before - top)
            peak[t] = top

        def weigh(i, t, slot):
            m, d = unit(i)
            p = jnp.exp2(bands(ring[i % RING]) - peak[t][None]).reshape(rows, rows).astype(bf16)
            v = jnp.concatenate([v_t[slot, 0], v_t[slot, 1]], 1)
            pltpu.matmul_push_rhs(p, staging_register=1, mxu_index=m)
            pltpu.matmul_acc_lhs(o_acc[m][d][0], v[:HEAD_DIM], load_staged_rhs=1)
            pltpu.matmul_acc_lhs(o_acc[m][d][1], v[HEAD_DIM:])

        def add(i, t, first):
            m, d = unit(i)
            new = pltpu.matmul_pop(o_acc[m][d][0])
            total = pltpu.matmul_pop(o_acc[m][d][1])[:8]
            if not first:
                scale = shrink[t]
                new = (bands(acc[t, :HEAD_DIM]) * scale[None]).reshape(HEAD_DIM, rows) + new
                total = acc[t, HEAD_DIM:] * scale + total
            acc[t, :HEAD_DIM] = new
            acc[t, HEAD_DIM:] = total

        pairs = lambda b: ((b, 0), (b, 1))
        lower = o * shared
        jobs = []
        for h in range(shared):
            jobs.append((shared + h, pairs(c), 0, True, True))
        for h in range(shared):
            jobs.append((h, pairs(partner), 1, True, True))
        for h in range(shared):
            jobs.append((lower + h, pairs(2 * chip), o, False, False))

        load_q.wait()
        prepare(1)
        turn(0, c, 0, c, 1)

        def meet():
            give_kv.wait_recv()
            give_q.wait_recv()
            prepare(0)
            turn(1, partner, 0, partner, 1)

        def start(i):
            if i == shared:
                meet()
            score(i, jobs[i][0], jobs[i][1])

        count = len(jobs)
        for i in range(AHEAD):
            start(i)
        for j in range(count + LAG + HOLD):
            k = j - LAG
            if 0 <= k - HOLD:
                add(k - HOLD, jobs[k - HOLD][0], jobs[k - HOLD][4])
            if 0 <= k < count:
                weigh(k, jobs[k][0], jobs[k][2])
            if j < count:
                collect(j, jobs[j][0], jobs[j][3], jobs[j][4])
            if j + AHEAD < count:
                start(j + AHEAD)

        for t in range(tiles - LAG - HOLD, tiles):
            shrink[t] = jnp.ones((8, rows), f32)
        for t in range(tiles - LAG, tiles):
            ring[t % RING] = jnp.full((rows, rows), MASKED, f32)

        def plan(r):
            e = lax.rem(r + o, 2)
            early = r < lax.select(chip == 3, 4, 2)
            b1 = lax.select(chip == 1, o, lax.select(chip == 2, lax.select(early, 1 - o, 2),
                                                     lax.select(early, 2 + e, 0)))
            b2 = lax.select(chip == 1, 1 - o, lax.select(chip == 2, lax.select(early, o, 3),
                                                         lax.select(early, 4 + e, 1)))
            h = lax.select(chip == 3, lax.select(early, r // 2, r - 4), lax.rem(r, 2))
            target = 2 * lax.select(chip == 3, 2, 3) + o
            onward = early & (r < 3)
            return b1, b2, h, onward, piece(b1, h, relay_sem.at[r], target)

        def result(t):
            scale = 1.0 / acc[t, HEAD_DIM:]
            x = (bands(acc[t, :HEAD_DIM]) * scale[None]).reshape(HEAD_DIM, rows)
            return x.T.astype(o_ref.dtype)

        def set_aside(h):
            stage[:, h * HEAD_DIM:(h + 1) * HEAD_DIM] = result(h)

        def keep(h):
            o_ref[:, head_cols(o * shared + h, HEAD_DIM)] = result(shared + h)

        ends = [shared * x // 8 for x in ENDS]
        begins = [0] + ends[:-1]

        def give(n, g):
            width = (ends[n] - begins[n]) * HEAD_DIM
            lo = begins[n] * HEAD_DIM
            cols = pl.ds(pl.multiple_of(g * span + lo, HEAD_DIM), width)
            src = stage.at[:, lo:lo + width]
            return remote(src, o_ref.at[:, cols], out_sem.at[0, n], out_sem.at[1, n], partner)

        def sweep(r, final):
            b1, b2, h, early, onward = plan(r)
            onward.wait_recv()
            pl.when(early)(onward.start)
            piece(b2, h, relay_sem.at[r], partner).wait_recv()
            slot = lax.rem(r, 2)
            turn(slot, b1, h, b2, h)
            keys = ((b1, h), (b2, h))
            for i in range(AHEAD):
                score(i, i, keys)
            for j in range(tiles):
                k = (j - LAG) % tiles
                n = (j - LAG - HOLD) % tiles
                weigh(k, k, slot if j >= LAG else 1 - slot)
                add(n, n, False)
                collect(j, j, False, False)
                if j + AHEAD < tiles:
                    score(j + AHEAD, j + AHEAD, keys)
                if final and j >= LAG + HOLD:
                    if n < shared:
                        set_aside(n)
                    else:
                        keep(n - shared)
                    if n + 1 in ends:
                        give(ends.index(n + 1), o).start()

        rounds = 2 * chip

        def body(r, carry):
            sweep(r, False)
            return carry

        @pl.when(chip > 0)
        def _():
            lax.fori_loop(0, rounds - 1, body, 0)
            send_late()
            sweep(rounds - 1, True)

        @pl.when(chip == 0)
        def _():
            for h in range(shared):
                set_aside(h)
            for h in range(tiles - LAG - HOLD - shared):
                keep(h)
            for n in range(len(ENDS)):
                give(n, o).start()

        last = lax.rem(rounds + 1, 2)
        for k in range(tiles - LAG, tiles):
            weigh(k, k, last)
            add(k - HOLD, k - HOLD, False)
            keep(k - HOLD - shared)
        for k in range(tiles - HOLD, tiles):
            add(k, k, False)
            keep(k - shared)

        def drain(r, carry):
            _, _, _, early, onward = plan(r)
            pl.when(early)(onward.wait_send)
            return carry

        lax.fori_loop(0, rounds, drain, 0)
        for n in range(len(ENDS)):
            give(n, 1 - o).wait_recv()
            give(n, o).wait_send()
        for wanted, copy in sends:
            pl.when(wanted)(copy.wait_send)
        give_q.wait_send()
        give_kv.wait_send()

    specs = [pltpu.ACC(m)((half, rows), f32) for m in range(2) for _ in range(4)]
    specs += [pltpu.ACC(m)((n, rows), f32) for m in range(2) for _ in range(2) for n in (HEAD_DIM, SUMS)]
    pl.run_scoped(pipeline, *specs)


def paired(rows, width, shared):
    half, tiles = rows // 2, 2 * shared
    bf16, f32, dma = jnp.bfloat16, jnp.float32, pltpu.SemaphoreType.DMA
    return pl.pallas_call(
        functools.partial(paired_kernel, shared),
        out_shape=pltpu.VMEM((rows, width), bf16),
        in_specs=[pl.BlockSpec(memory_space=pltpu.HBM)] * 3,
        out_specs=pl.BlockSpec(memory_space=pltpu.VMEM),
        scratch_shapes=[
            pltpu.VMEM((2, rows, shared * HEAD_DIM), bf16),
            pltpu.VMEM((tiles, 2, 2 * HEAD_DIM, half), bf16),
            pltpu.VMEM((8, 2, 2, half, HEAD_DIM), bf16),
            pltpu.VMEM((2, 2, half, HEAD_DIM), bf16),
            pltpu.VMEM((tiles, HEAD_DIM + 8, rows), f32),
            pltpu.VMEM((tiles, 8, rows), f32),
            pltpu.VMEM((tiles, 8, rows), f32),
            pltpu.VMEM((RING, rows, rows), f32),
            pltpu.VMEM((2, 2, HEAD_DIM + SUMS, half), bf16),
            pltpu.VMEM((rows, shared * HEAD_DIM), bf16),
            dma((9,)), dma((4,)), dma((3, 4)), dma((6,)), dma((8, 2)), dma((2, len(ENDS))),
        ],
        compiler_params=pltpu.CompilerParams(
            collective_id=1, has_side_effects=True, vmem_limit_bytes=60 * 1024 * 1024))


def solution(mesh):
    nc = mesh.shape["ctx"]

    def step(queries, keys, values):
        rows, width = queries.shape
        per_dev = width // HEAD_DIM
        group = HEADS // KV_HEADS
        kv_dev = per_dev // min(group, per_dev)
        if nc == 8 and kv_dev == 2 and rows == 2 * HEAD_DIM and per_dev == 2 * group:
            return paired(rows, width, group)(queries, keys, values)
        any_space = pl.BlockSpec(memory_space=pltpu.HBM)
        return pl.pallas_call(
            functools.partial(kernel, nc, per_dev, group, kv_dev),
            out_shape=pltpu.VMEM((rows, width), jnp.bfloat16),
            in_specs=[any_space] * 3,
            out_specs=pl.BlockSpec(memory_space=pltpu.VMEM),
            scratch_shapes=[
                pltpu.VMEM((rows, width), jnp.bfloat16),
                pltpu.VMEM((nc, kv_dev, 2, rows, HEAD_DIM), jnp.bfloat16),
                pltpu.VMEM((per_dev, rows, 2 * LANES), jnp.float32),
                pltpu.VMEM((per_dev, rows, LANES), jnp.float32),
                pltpu.SemaphoreType.DMA((2 * kv_dev + 1,)),
                pltpu.SemaphoreType.DMA((nc // 2, kv_dev)),
                pltpu.SemaphoreType.DMA((nc // 2, kv_dev)),
                pltpu.SemaphoreType.DMA((nc // 2, kv_dev)),
                pltpu.SemaphoreType.DMA((nc, kv_dev)),
            ],
            compiler_params=pltpu.CompilerParams(
                collective_id=0, has_side_effects=True, vmem_limit_bytes=60 * 1024 * 1024),
        )(queries, keys, values)

    return jax.shard_map(
        step, mesh=mesh,
        in_specs=(P("ctx", "tp"), P("ctx", None), P("ctx", None)),
        out_specs=P("ctx", "tp"), check_vma=False)
```

```python
import functools
import math

import jax
import jax.numpy as jnp
from jax import lax
from jax.experimental import pallas as pl
from jax.experimental.pallas import tpu as pltpu
from jax.sharding import PartitionSpec as P

HEADS = 64
KV_HEADS = 8
HEAD_DIM = 128
LANES = 128
MASKED = -1e30
CHUNK = 8
DEPTH = 1
ROUTED = 1
EXP2_SCALE = HEAD_DIM ** -0.5 * math.log2(math.e)


def attend_heads(q_v, kv, acc, peak, heads, kv_head, blocks, masked, first):
    k = jnp.concatenate([kv[b, kv_head, 0] for b in blocks], 0)
    v = jnp.concatenate([kv[b, kv_head, 1] for b in blocks], 0)
    v = jnp.concatenate([v, jnp.ones((v.shape[0], LANES), v.dtype)], 1)
    rows, count = q_v.shape[0], k.shape[0]

    def score(h):
        q = q_v[:, pl.ds(pl.multiple_of(h * HEAD_DIM, HEAD_DIM), HEAD_DIM)]
        return lax.dot_general(q, k, (((1,), (1,)), ((), ())), preferred_element_type=jnp.float32)

    def fold(h, s):
        if masked:
            row = lax.broadcasted_iota(jnp.int32, s.shape, 0)
            col = lax.broadcasted_iota(jnp.int32, s.shape, 1)
            s = jnp.where(col <= row, s, MASKED)
        top = jnp.broadcast_to(jnp.max(s, axis=1, keepdims=True), (rows, LANES))
        if not first:
            before = peak[h]
            top = jnp.maximum(before, top)
        peak[h] = top
        wide = jnp.concatenate([top] * (count // LANES), 1)
        w = jnp.exp2((s - wide) * EXP2_SCALE).astype(jnp.bfloat16)
        new = jnp.dot(w, v, preferred_element_type=jnp.float32)
        if not first:
            shrink = jnp.exp2((before - top) * EXP2_SCALE)
            new = acc[h] * jnp.concatenate([shrink, shrink], 1) + new
        acc[h] = new

    ahead = [score(h) for h in heads[:DEPTH]]
    for i, h in enumerate(heads):
        if i + DEPTH < len(heads):
            ahead.append(score(heads[i + DEPTH]))
        fold(h, ahead.pop(0))


def kernel(nc, per_dev, group, kv_dev, q_hbm, k_hbm, v_hbm, o_ref,
           q_v, kv, acc, peak, loc_sem, send_sem, fwd_sem, far_sem, recv_sem):
    c = lax.axis_index("ctx")
    tp = lax.axis_index("tp")
    odd = lax.rem(c, 2)
    pair = c // 2
    partner = c + 1 - 2 * odd
    shared = per_dev // kv_dev
    chunk = min(CHUNK, shared)
    square = nc == 8 and kv_dev == 2
    base = tp * per_dev // group

    loads = []
    for g in range(kv_dev):
        cols = pl.ds(pl.multiple_of((base + g) * HEAD_DIM, HEAD_DIM), HEAD_DIM)
        loads.append([
            pltpu.make_async_copy(ref.at[:, cols], kv.at[c, g, i], loc_sem.at[2 * g + i])
            for i, ref in enumerate((k_hbm, v_hbm))])
        for load in loads[g]:
            load.start()
    load_q = pltpu.make_async_copy(q_hbm, q_v, loc_sem.at[2 * kv_dev])
    load_q.start()

    barrier = pltpu.get_barrier_semaphore()
    pl.semaphore_signal(barrier, inc=1, device_id={"ctx": partner})
    for i in range(1, nc // 2):
        pl.semaphore_signal(barrier, inc=1, device_id={"ctx": lax.rem(c + 2 * i, nc)})
    pl.semaphore_wait(barrier, nc // 2)

    def copy_to(b, g, target, sem):
        return pltpu.make_async_remote_copy(
            src_ref=kv.at[b, g], dst_ref=kv.at[b, g], send_sem=sem, recv_sem=recv_sem.at[b, g],
            device_id={"ctx": target})

    for load in sum(loads, []):
        load.wait()
    sends, late = [], []
    for g in range(kv_dev):
        sends.append((odd == 0, copy_to(c, g, partner, send_sem.at[0, g])))
        if square:
            beside = copy_to(c, g, lax.rem(c + 2, nc), send_sem.at[1, g])
            sends.append((lax.rem(pair, 2) == 0, beside))
            if g >= ROUTED:
                late.append(beside)
            first = kv_dev - 1 - g
            other = lax.select(pair == 0, first, g)
            sends.append((pair < 2, copy_to(c, other, lax.rem(c + 4, nc), send_sem.at[2, g])))
        else:
            for i in range(1, nc // 2):
                sends.append((c + 2 * i < nc, copy_to(c, g, lax.rem(c + 2 * i, nc), send_sem.at[i, g])))
    for wanted, copy in sends:
        pl.when(wanted)(copy.start)
    load_q.wait()

    def item(t):
        if not square:
            return pair - 1 - t // kv_dev, lax.rem(t, kv_dev)
        third = (lax.select(t < 4, 2 - lax.rem(t, 2), 0), lax.select(t < 4, t // 2, t - 4))
        second = (t // 2, lax.rem((t + 1) // 2 + 1, 2))
        return (lax.select(pair == 3, third[0], lax.select(pair == 2, second[0], 0)),
                lax.select(pair == 3, third[1], lax.select(pair == 2, second[1], t)))

    def onward(p, g):
        mine = 2 * p + odd
        up = ((pair == 1) & (g == 0)) | ((pair == 2) & (p == 0) & (g == 1))
        back = (pair == 3) & (p == 1) & (g < ROUTED)
        target = lax.select(pair == 3, 4 + odd, 6 + odd)
        return up | back, copy_to(mine, g, target, far_sem.at[p, g])

    def pull(t):
        p, g = item(t)
        copy = copy_to(2 * p + odd, g, partner, fwd_sem.at[p, g])
        copy.wait_recv()
        if square:
            wanted, far = onward(p, g)
            pl.when(wanted)(far.start)
        copy.start()

    def sweep(blocks, kv_head, masked, first):
        def body(n, carry):
            heads = [n * chunk + i for i in range(chunk)]
            g = n * chunk // shared if kv_head is None else kv_head
            attend_heads(q_v, kv, acc, peak, heads, g, blocks, masked, first)
            return carry
        return body

    def finish(g, carry):
        for i in range(shared):
            h = g * shared + i
            out = acc[h, :, :LANES] / acc[h, :, LANES:]
            o_ref[:, pl.ds(pl.multiple_of(h * HEAD_DIM, HEAD_DIM), HEAD_DIM)] = out.astype(o_ref.dtype)
        return carry

    chunks = per_dev // chunk
    steps = pair * kv_dev
    lax.fori_loop(0, chunks, sweep([c], None, True, True), 0)

    if square:
        for copy in late:
            pl.when(pair == 1)(copy.start)

    def first_pulls():
        pull(0)
        if square:
            pl.when(pair == 3)(functools.partial(pull, 1))

    @pl.when(odd == 1)
    def _():
        for g in range(kv_dev):
            copy_to(c - 1, g, partner, send_sem.at[0, g]).wait_recv()
        work = sweep([c - 1], None, False, False)

        def body(n, carry):
            pl.when((n == chunks // 2) & (pair > 0))(first_pulls)
            return work(n, carry)

        lax.fori_loop(0, chunks, body, 0)

    pl.when((odd == 0) & (pair > 0))(first_pulls)

    def step(t, carry):
        p, g = item(t)
        copy_to(2 * p + 1 - odd, g, partner, fwd_sem.at[p, g]).wait_recv()
        body = sweep([2 * p, 2 * p + 1], g, False, False)

        done = (pair == 3) & (t == 0) if square else False

        @pl.when((t + 1 < steps) & jnp.logical_not(done))
        def _():
            pull(t + 1)

        per_head = shared // chunk
        lax.fori_loop(g * per_head, (g + 1) * per_head, body, 0)

        @pl.when(t >= steps - kv_dev)
        def _():
            finish(g, 0)
        return carry

    lax.fori_loop(0, steps, step, 0)

    @pl.when(pair == 0)
    def _():
        lax.fori_loop(0, kv_dev, finish, 0)

    def drain(t, carry):
        p, g = item(t)
        copy_to(2 * p + odd, g, partner, fwd_sem.at[p, g]).wait_send()
        if square:
            wanted, far = onward(p, g)
            pl.when(wanted)(far.wait_send)
        return carry

    lax.fori_loop(0, steps, drain, 0)
    for wanted, copy in sends:
        pl.when(wanted)(copy.wait_send)
    for copy in late:
        pl.when(pair == 1)(copy.wait_send)


AHEAD = 4
LAG = 3
HOLD = 3
RING = 8
SUMS = 16
ENDS = (4, 7, 8)


def paired_kernel(shared, q_hbm, k_hbm, v_hbm, o_ref, q_raw, q_t, kv, other, acc, peak, shrink,
                  ring, v_t, stage, load_sem, pair_sem, send_sem, relay_sem, recv_sem, out_sem):
    c = lax.axis_index("ctx")
    tp = lax.axis_index("tp")
    o = lax.rem(c, 2)
    chip = c // 2
    partner = c + 1 - 2 * o
    rows = q_raw.shape[1]
    half = rows // 2
    span = shared * HEAD_DIM
    tiles = 2 * shared
    f32, bf16 = jnp.float32, jnp.bfloat16

    def head_cols(g, width):
        return pl.ds(pl.multiple_of(g * width, width), width)

    loads = []
    for h in range(2):
        for i, ref in enumerate((k_hbm, v_hbm)):
            for n, (g, dst) in enumerate(((o, kv.at[c, h, i]), (1 - o, other.at[h, i]))):
                src = ref.at[pl.ds(h * half, half), head_cols(2 * tp + g, HEAD_DIM)]
                loads.append(pltpu.make_async_copy(src, dst, load_sem.at[4 * h + 2 * i + n]))
    barrier = pltpu.get_barrier_semaphore()
    beside = 2 * (chip + 1 - 2 * lax.rem(chip, 2))
    across = 2 * lax.rem(chip + 2, 4)
    for target in (partner, beside, beside + 1, across, across + 1):
        pl.semaphore_signal(barrier, inc=1, device_id={"ctx": target})
    middle = (chip == 1) | (chip == 2)
    opposite = 2 * (3 - chip)

    @pl.when(middle)
    def _():
        for target in (opposite, opposite + 1):
            pl.semaphore_signal(barrier, inc=1, device_id={"ctx": target})

    for load in loads:
        load.start()
    load_q = pltpu.make_async_copy(q_hbm.at[:, head_cols(o, span)], q_raw.at[1], load_sem.at[8])
    load_q.start()

    v_t[...] = jnp.ones(v_t.shape, bf16)
    pl.semaphore_wait(barrier, lax.select(middle, 7, 5))

    def remote(src, dst, send, recv, target):
        return pltpu.make_async_remote_copy(
            src_ref=src, dst_ref=dst, send_sem=send, recv_sem=recv, device_id={"ctx": target})

    def piece(b, h, send, target):
        return remote(kv.at[b, h], kv.at[b, h], send, recv_sem.at[b, h], target)

    give_q = remote(q_hbm.at[:, head_cols(1 - o, span)], q_raw.at[0], pair_sem.at[0], pair_sem.at[1], partner)
    give_kv = remote(other, kv.at[c], pair_sem.at[2], pair_sem.at[3], partner)
    for load in loads:
        load.wait()
    sends = []
    for n, (wanted, base, flip) in enumerate((
            ((chip == 0) | (chip == 2), beside, 0), (chip < 2, across, 1))):
        for k, (h, swap) in enumerate(((0, 0), (0, 1), (1, 0), (1, 1))):
            sem = send_sem.at[n, k]
            same = piece(c, h, sem, base + o)
            cross = remote(other.at[h], kv.at[c, h], sem, recv_sem.at[c, h], base + 1 - o)
            if flip:
                first, then = (same, cross), (cross, same)
                sends.append((wanted & (chip == 1), first[swap]))
                sends.append((wanted & (chip == 0), then[swap]))
            else:
                sends.append((wanted, (same, cross)[swap]))
    for wanted, copy in sends:
        pl.when(wanted)(copy.start)
    give_q.start()
    give_kv.start()
    late = [remote(other.at[1], kv.at[c, 1], send_sem.at[2, 1], recv_sem.at[c, 1], opposite + 1 - o)]
    sends += [(chip == 1, copy) for copy in late]

    def send_late():
        for copy in late:
            pl.when(chip == 1)(copy.start)

    def prepare(slot):
        for h in range(shared):
            x = q_raw[slot, :, h * HEAD_DIM:(h + 1) * HEAD_DIM].astype(f32) * EXP2_SCALE
            x = x.T
            top = x.astype(bf16)
            low = (x - top.astype(f32)).astype(bf16)
            for s in range(2):
                cols = slice(s * half, (s + 1) * half)
                q_t[slot * shared + h, s, :HEAD_DIM] = top[:, cols]
                q_t[slot * shared + h, s, HEAD_DIM:] = low[:, cols]

    def turn(slot, b1, h1, b2, h2):
        for s, (b, h) in enumerate(((b1, h1), (b2, h2))):
            v_t[slot, s, :HEAD_DIM] = kv[b, h, 1].astype(f32).T.astype(bf16)

    def bands(x):
        return x.reshape(x.shape[0] // 8, 8, rows)

    def pipeline(*accs):
        accs = iter(accs)
        s_acc = [[[next(accs) for _ in range(2)] for _ in range(2)] for _ in range(2)]
        o_acc = [[[next(accs) for _ in range(2)] for _ in range(2)] for _ in range(2)]

        def unit(i):
            return i % 2, i // 2 % 2

        def score(i, t, keys):
            m, d = unit(i)
            q = jnp.concatenate([q_t[t, 0], q_t[t, 1]], 1)
            pltpu.matmul_push_rhs(q, staging_register=0, mxu_index=m)
            for s, (b, h) in enumerate(keys):
                k = kv[b, h, 0]
                pltpu.matmul_acc_lhs(s_acc[m][d][s], jnp.concatenate([k, k], 1),
                                     load_staged_rhs=None if s else 0)

        def collect(i, t, masked, first):
            m, d = unit(i)
            top = None
            for s in range(2):
                x = pltpu.matmul_pop(s_acc[m][d][s])
                if masked:
                    key = lax.broadcasted_iota(jnp.int32, x.shape, 0) + s * half
                    row = lax.broadcasted_iota(jnp.int32, x.shape, 1)
                    x = jnp.where(key <= row, x, MASKED)
                ring[i % RING, s * half:(s + 1) * half] = x
                most = jnp.max(bands(x), 0)
                top = most if top is None else jnp.maximum(top, most)
            top = jnp.broadcast_to(jnp.max(top, 0, keepdims=True), (8, rows))
            if not first:
                before = peak[t]
                top = jnp.maximum(before, top)
                shrink[t] = jnp.exp2(before - top)
            peak[t] = top

        def weigh(i, t, slot):
            m, d = unit(i)
            p = jnp.exp2(bands(ring[i % RING]) - peak[t][None]).reshape(rows, rows).astype(bf16)
            v = jnp.concatenate([v_t[slot, 0], v_t[slot, 1]], 1)
            pltpu.matmul_push_rhs(p, staging_register=1, mxu_index=m)
            pltpu.matmul_acc_lhs(o_acc[m][d][0], v[:HEAD_DIM], load_staged_rhs=1)
            pltpu.matmul_acc_lhs(o_acc[m][d][1], v[HEAD_DIM:])

        def add(i, t, first):
            m, d = unit(i)
            new = pltpu.matmul_pop(o_acc[m][d][0])
            total = pltpu.matmul_pop(o_acc[m][d][1])[:8]
            if not first:
                scale = shrink[t]
                new = (bands(acc[t, :HEAD_DIM]) * scale[None]).reshape(HEAD_DIM, rows) + new
                total = acc[t, HEAD_DIM:] * scale + total
            acc[t, :HEAD_DIM] = new
            acc[t, HEAD_DIM:] = total

        pairs = lambda b: ((b, 0), (b, 1))
        lower = o * shared
        jobs = []
        for h in range(shared):
            jobs.append((shared + h, pairs(c), 0, True, True))
        for h in range(shared):
            jobs.append((h, pairs(partner), 1, True, True))
        for h in range(shared):
            jobs.append((lower + h, pairs(2 * chip), o, False, False))

        load_q.wait()
        prepare(1)
        turn(0, c, 0, c, 1)

        def meet():
            give_kv.wait_recv()
            give_q.wait_recv()
            prepare(0)
            turn(1, partner, 0, partner, 1)

        def start(i):
            if i == shared:
                meet()
            score(i, jobs[i][0], jobs[i][1])

        count = len(jobs)
        for i in range(AHEAD):
            start(i)
        for j in range(count + LAG + HOLD):
            k = j - LAG
            if 0 <= k - HOLD:
                add(k - HOLD, jobs[k - HOLD][0], jobs[k - HOLD][4])
            if 0 <= k < count:
                weigh(k, jobs[k][0], jobs[k][2])
            if j < count:
                collect(j, jobs[j][0], jobs[j][3], jobs[j][4])
            if j + AHEAD < count:
                start(j + AHEAD)

        for t in range(tiles - LAG - HOLD, tiles):
            shrink[t] = jnp.ones((8, rows), f32)
        for t in range(tiles - LAG, tiles):
            ring[t % RING] = jnp.full((rows, rows), MASKED, f32)

        def plan(r):
            e = lax.rem(r + o, 2)
            early = r < lax.select(chip == 3, 4, 2)
            b1 = lax.select(chip == 1, o, lax.select(chip == 2, lax.select(early, 1 - o, 2),
                                                     lax.select(early, 2 + e, 0)))
            b2 = lax.select(chip == 1, 1 - o, lax.select(chip == 2, lax.select(early, o, 3),
                                                         lax.select(early, 4 + e, 1)))
            h = lax.select(chip == 3, lax.select(early, r // 2, r - 4), lax.rem(r, 2))
            target = 2 * lax.select(chip == 3, 2, 3) + o
            onward = early & (r < 3)
            return b1, b2, h, onward, piece(b1, h, relay_sem.at[r], target)

        def result(t):
            scale = 1.0 / acc[t, HEAD_DIM:]
            x = (bands(acc[t, :HEAD_DIM]) * scale[None]).reshape(HEAD_DIM, rows)
            return x.T.astype(o_ref.dtype)

        def set_aside(h):
            stage[:, h * HEAD_DIM:(h + 1) * HEAD_DIM] = result(h)

        def keep(h):
            o_ref[:, head_cols(o * shared + h, HEAD_DIM)] = result(shared + h)

        ends = [shared * x // 8 for x in ENDS]
        begins = [0] + ends[:-1]

        def give(n, g):
            width = (ends[n] - begins[n]) * HEAD_DIM
            lo = begins[n] * HEAD_DIM
            cols = pl.ds(pl.multiple_of(g * span + lo, HEAD_DIM), width)
            src = stage.at[:, lo:lo + width]
            return remote(src, o_ref.at[:, cols], out_sem.at[0, n], out_sem.at[1, n], partner)

        def sweep(r, final):
            b1, b2, h, early, onward = plan(r)
            onward.wait_recv()
            pl.when(early)(onward.start)
            piece(b2, h, relay_sem.at[r], partner).wait_recv()
            slot = lax.rem(r, 2)
            turn(slot, b1, h, b2, h)
            keys = ((b1, h), (b2, h))
            for i in range(AHEAD):
                score(i, i, keys)
            for j in range(tiles):
                k = (j - LAG) % tiles
                n = (j - LAG - HOLD) % tiles
                weigh(k, k, slot if j >= LAG else 1 - slot)
                add(n, n, False)
                collect(j, j, False, False)
                if j + AHEAD < tiles:
                    score(j + AHEAD, j + AHEAD, keys)
                if final and j >= LAG + HOLD:
                    if n < shared:
                        set_aside(n)
                    else:
                        keep(n - shared)
                    if n + 1 in ends:
                        give(ends.index(n + 1), o).start()

        rounds = 2 * chip

        def body(r, carry):
            sweep(r, False)
            return carry

        @pl.when(chip > 0)
        def _():
            lax.fori_loop(0, rounds - 1, body, 0)
            send_late()
            sweep(rounds - 1, True)

        @pl.when(chip == 0)
        def _():
            for h in range(shared):
                set_aside(h)
            for h in range(tiles - LAG - HOLD - shared):
                keep(h)
            for n in range(len(ENDS)):
                give(n, o).start()

        last = lax.rem(rounds + 1, 2)
        for k in range(tiles - LAG, tiles):
            weigh(k, k, last)
            add(k - HOLD, k - HOLD, False)
            keep(k - HOLD - shared)
        for k in range(tiles - HOLD, tiles):
            add(k, k, False)
            keep(k - shared)

        def drain(r, carry):
            _, _, _, early, onward = plan(r)
            pl.when(early)(onward.wait_send)
            return carry

        lax.fori_loop(0, rounds, drain, 0)
        for n in range(len(ENDS)):
            give(n, 1 - o).wait_recv()
            give(n, o).wait_send()
        for wanted, copy in sends:
            pl.when(wanted)(copy.wait_send)
        give_q.wait_send()
        give_kv.wait_send()

    specs = [pltpu.ACC(m)((half, rows), f32) for m in range(2) for _ in range(4)]
    specs += [pltpu.ACC(m)((n, rows), f32) for m in range(2) for _ in range(2) for n in (HEAD_DIM, SUMS)]
    pl.run_scoped(pipeline, *specs)


def paired(rows, width, shared):
    half, tiles = rows // 2, 2 * shared
    bf16, f32, dma = jnp.bfloat16, jnp.float32, pltpu.SemaphoreType.DMA
    return pl.pallas_call(
        functools.partial(paired_kernel, shared),
        out_shape=pltpu.VMEM((rows, width), bf16),
        in_specs=[pl.BlockSpec(memory_space=pltpu.HBM)] * 3,
        out_specs=pl.BlockSpec(memory_space=pltpu.VMEM),
        scratch_shapes=[
            pltpu.VMEM((2, rows, shared * HEAD_DIM), bf16),
            pltpu.VMEM((tiles, 2, 2 * HEAD_DIM, half), bf16),
            pltpu.VMEM((8, 2, 2, half, HEAD_DIM), bf16),
            pltpu.VMEM((2, 2, half, HEAD_DIM), bf16),
            pltpu.VMEM((tiles, HEAD_DIM + 8, rows), f32),
            pltpu.VMEM((tiles, 8, rows), f32),
            pltpu.VMEM((tiles, 8, rows), f32),
            pltpu.VMEM((RING, rows, rows), f32),
            pltpu.VMEM((2, 2, HEAD_DIM + SUMS, half), bf16),
            pltpu.VMEM((rows, shared * HEAD_DIM), bf16),
            dma((9,)), dma((4,)), dma((3, 4)), dma((6,)), dma((8, 2)), dma((2, len(ENDS))),
        ],
        compiler_params=pltpu.CompilerParams(
            collective_id=1, has_side_effects=True, vmem_limit_bytes=60 * 1024 * 1024))


def solution(mesh):
    nc = mesh.shape["ctx"]

    def step(queries, keys, values):
        rows, width = queries.shape
        per_dev = width // HEAD_DIM
        group = HEADS // KV_HEADS
        kv_dev = per_dev // min(group, per_dev)
        if nc == 8 and kv_dev == 2 and rows == 2 * HEAD_DIM and per_dev == 2 * group:
            return paired(rows, width, group)(queries, keys, values)
        any_space = pl.BlockSpec(memory_space=pltpu.HBM)
        return pl.pallas_call(
            functools.partial(kernel, nc, per_dev, group, kv_dev),
            out_shape=pltpu.VMEM((rows, width), jnp.bfloat16),
            in_specs=[any_space] * 3,
            out_specs=pl.BlockSpec(memory_space=pltpu.VMEM),
            scratch_shapes=[
                pltpu.VMEM((rows, width), jnp.bfloat16),
                pltpu.VMEM((nc, kv_dev, 2, rows, HEAD_DIM), jnp.bfloat16),
                pltpu.VMEM((per_dev, rows, 2 * LANES), jnp.float32),
                pltpu.VMEM((per_dev, rows, LANES), jnp.float32),
                pltpu.SemaphoreType.DMA((2 * kv_dev + 1,)),
                pltpu.SemaphoreType.DMA((nc // 2, kv_dev)),
                pltpu.SemaphoreType.DMA((nc // 2, kv_dev)),
                pltpu.SemaphoreType.DMA((nc // 2, kv_dev)),
                pltpu.SemaphoreType.DMA((nc, kv_dev)),
            ],
            compiler_params=pltpu.CompilerParams(
                collective_id=0, has_side_effects=True, vmem_limit_bytes=60 * 1024 * 1024),
        )(queries, keys, values)

    return jax.shard_map(
        step, mesh=mesh,
        in_specs=(P("ctx", "tp"), P("ctx", None), P("ctx", None)),
        out_specs=P("ctx", "tp"), check_vma=False)
```
